32 devices in a mesh: groups: 2 (over x), img: 8 (over z, y), space: 2 (over core).
Axes of the slice: x: 2, y: 2, z: 4, core: 2. Of those that a mesh axis runs over, the one named last changes fastest.
Arguments:
- path: float32 [64, 64, 4096], P(('groups', 'img'), 'space'), parts along dimension 0, may hold values from -3 to 3
- bracket: int32 [64], P(('groups', 'img')), parts along dimension 0, may hold values from 0 to 30, as said below
Outputs:
- new_path: float32 [64, 64, 4096], P(('groups', 'img'), 'space'), parts along dimension 0
The draws below stay inside these ranges and needn't reach their ends.
There are 2 independent parts, one for each index of `groups`. The reference program is written for one: setup_inputs(seed, part) draws one part's arguments, and reference() takes and returns one part's arrays. A program takes and returns all parts, laid end to end along the dimension named above; each array names one. Nothing has to cross between parts.
Inputs may be any that keep to these rules, and one draw needn't show every extreme that they name: bracket[j] differs from j by at most 2; it is given, not derived from the arc lengths, so the target arc length of image j need not lie between arc_b and arc_(b+1).
All inputs are finite; a program needn't handle non-finite values.
Results may differ from the reference program's by a relative error of at most 0.0003.
Values sent between devices are 32-bit elements; how exact they have to be, the bound alone decides.
No kernel may reach another device: no remote copies, remote signals or barrier semaphores. Data moves between devices by JAX's collectives and lax.ppermute only.
A program may use at most 64 MiB of HBM per device.

```python
import jax
import jax.numpy as jnp
from jax import lax

COLS = 4096
REACH = 2
ITERS = 2
IMAGES = 32
GRID_ROWS = 64


def draw_bracket(key, part):
    offsets = jax.random.randint(jax.random.fold_in(key, 7), (IMAGES,), -REACH, REACH + 1)
    return jnp.clip(jnp.arange(IMAGES) + offsets, 0, IMAGES - 2).astype(jnp.int32)


def levels(rng, extent, pieces, smallest, high):
    loudness = 1.0
    for position, parts in pieces:
        steps = jax.random.uniform(jax.random.fold_in(jax.random.fold_in(rng, 6), position), (parts,), jnp.float32, smallest / len(pieces), high / len(pieces))
        loudness = loudness * jnp.repeat(jnp.exp(steps), extent[position] // parts).reshape((-1,) + (1,) * (len(extent) - 1 - position))
    return loudness


def bell_draw(own_key, dims, scale, limit, pieces=(), held_as=jnp.bfloat16):
    array = jax.random.normal(own_key, dims, jnp.float32) * scale
    if len(pieces) > 0:
        array = levels(own_key, dims, pieces, -0.22, 0.18) * array
    return jnp.clip(array, min=-limit, max=limit).astype(held_as)


def setup_inputs(seed: int = 0, part: int = 0) -> dict:
    keys = jax.random.split(jax.random.key(seed), 3)
    part_splits = jax.random.split(jax.random.fold_in(keys[2], part), 3)
    path = bell_draw(part_splits[0], (IMAGES, GRID_ROWS, COLS), 0.5, 3.0, ((0, 8), (1, 2)), jnp.float32)
    bracket = draw_bracket(jax.random.fold_in(jax.random.fold_in(keys[2], part), 71), part)
    return {"path": path, "bracket": bracket}


TIME_STEP = 0.002
EPSILON = 1e-06

def laplace(field):
    return jnp.roll(field, 1, -2) + jnp.roll(field, -1, -2) + jnp.roll(field, 1, -1) + jnp.roll(field, -1, -1) - 4.0 * field

def along_path(field, count):
    ids = jnp.arange(count)
    is_first = (ids == 0)[:, None, None]
    is_last = (ids == count - 1)[:, None, None]
    earlier = jnp.concatenate([field[:1], field[:-1]], axis=0)
    following = jnp.concatenate([field[1:], field[-1:]], axis=0)
    stretch = jnp.where(is_first | is_last, jnp.float32(count - 1), jnp.float32((count - 1) / 2.0))
    return (following - earlier) * stretch

def iterate(images, count):
    tangent = along_path(images, count)
    drift_v = laplace(images) + images - images ** 3
    speed = jnp.sqrt(lax.optimization_barrier(jnp.sum(drift_v * drift_v, axis=(1, 2))) + EPSILON) / jnp.sqrt(lax.optimization_barrier(jnp.sum(tangent * tangent, axis=(1, 2))) + EPSILON)
    theta = speed[:, None, None] * tangent - drift_v
    descent = speed[:, None, None] * along_path(theta, count) + laplace(theta) + (1.0 - 3.0 * images * images) * theta
    ids = jnp.arange(count)
    inside = ((ids > 0) & (ids < count - 1))[:, None, None]
    return images + TIME_STEP * jnp.where(inside, descent, 0.0)

def reference(path, bracket):
    count = path.shape[0]
    images = path
    for iteration in range(ITERS):
        images = iterate(images, count)
    diffs = images[1:] - images[:-1]
    segments = jnp.sqrt(lax.optimization_barrier(jnp.sum(diffs * diffs, axis=(1, 2))) + EPSILON)
    seg_full = jnp.concatenate([jnp.zeros((1,), segments.dtype), segments])
    arc = jnp.cumsum(seg_full)
    length = arc[-1]
    target = length * jnp.arange(count).astype(segments.dtype) / (count - 1)
    lower = bracket.astype(jnp.int32)
    weight = (target - arc[lower]) / seg_full[lower + 1]
    base = images[lower]
    return base + weight[:, None, None] * (images[lower + 1] - base)
```

```python
import functools

import jax
import jax.numpy as jnp
from jax import lax
from jax.experimental import pallas as pl
from jax.experimental.pallas import tpu as pltpu
from jax.sharding import PartitionSpec as P

REACH = 2
ITERS = 2
TIME_STEP = 0.002
EPSILON = 1e-06

LANES = 128
SUBLANES = 8
PAIR = 2
LOW = 2 * ITERS + 1
HIGH = 2 * ITERS
EDGE = 2 * ITERS
VMEM_LIMIT = 28 * 1024 * 1024

F32 = jnp.float32


def call(kernel, out_shapes, scratch=(), smem=0, operands=0, aliases=None):
    specs = [pl.BlockSpec(memory_space=pltpu.SMEM)] * smem
    specs += [pl.BlockSpec(memory_space=pltpu.VMEM)] * operands
    return pl.pallas_call(
        kernel,
        out_shape=out_shapes,
        in_specs=specs,
        out_specs=jax.tree.map(lambda _: pl.BlockSpec(memory_space=pltpu.VMEM), out_shapes),
        scratch_shapes=list(scratch),
        compiler_params=pltpu.CompilerParams(vmem_limit_bytes=VMEM_LIMIT),
    )


def pair_position():
    index = lax.axis_index("img")
    return lax.div(index, PAIR), lax.rem(index, PAIR)


def swap_pairs(value):
    count = lax.axis_size("img")
    return lax.ppermute(value, "img", [(i, i ^ 1) for i in range(count)])


def small_sum(value, steps):
    size = lax.axis_size("space")
    if size & (size - 1) == 0:
        step = 1
        while step < size:
            value = value + lax.ppermute(value, "space", [(i, i ^ step) for i in range(size)])
            step *= 2
    else:
        value = lax.psum(value, "space")
    count = lax.axis_size("img")
    for step in steps:
        value = value + lax.ppermute(value, "img", [(i, i ^ step) for i in range(count)])
    return value


def neighbour_rows(block):
    size = lax.axis_size("space")
    top, bottom = block[:, :EDGE], block[:, -EDGE:]
    if size == 1:
        return jnp.concatenate([top, bottom], axis=1)
    if size == 2:
        return lax.ppermute(jnp.concatenate([top, bottom], axis=1), "space", [(0, 1), (1, 0)])
    after = lax.ppermute(top, "space", [(i, (i - 1) % size) for i in range(size)])
    before = lax.ppermute(bottom, "space", [(i, (i + 1) % size) for i in range(size)])
    return jnp.concatenate([after, before], axis=1)


def pack_kernel(x_ref, keep_ref, send_ref):
    _, lo = pair_position()
    columns = x_ref.shape[2]
    half = columns // PAIR
    lane = lax.broadcasted_iota(jnp.int32, (x_ref.shape[1], LANES), 1)

    def body(k, carry):
        for ref, part in ((keep_ref, lo), (send_ref, 1 - lo)):
            begin = pl.multiple_of(part * half, LANES)
            right = pl.multiple_of((1 - part) * half, LANES)
            left = pl.multiple_of((1 - part) * half + half - LANES, LANES)
            ref[k, :, 0:half] = x_ref[k, :, pl.ds(begin, half)]
            ref[k, :, half:] = jnp.where(
                lane < LANES // 2, x_ref[k, :, pl.ds(right, LANES)], x_ref[k, :, pl.ds(left, LANES)]
            )
        return carry

    lax.fori_loop(0, x_ref.shape[0], body, 0)


def sum_of_neighbours(load, tiles, rows, use):
    lane = lax.broadcasted_iota(jnp.int32, (rows, LANES), 1)
    is_first, is_last = lane == 0, lane == LANES - 1
    center = load(0)
    from_left = pltpu.roll(load(tiles - 1), 1, 1)
    to_left = pltpu.roll(center, LANES - 1, 1)
    for t in range(tiles):
        following = load((t + 1) % tiles)
        shifted = pltpu.roll(center, 1, 1)
        next_to_left = pltpu.roll(following, LANES - 1, 1)
        west = jnp.where(is_first, from_left, shifted)
        east = jnp.where(is_last, next_to_left, to_left)
        north = pltpu.roll(center, 1, 0)
        south = pltpu.roll(center, rows - 1, 0)
        use(t, center, (north + south) + (west + east))
        center, from_left, to_left = following, shifted, next_to_left


def tile_of(t):
    return slice(t * LANES, (t + 1) * LANES)


def neighbours_of(k, first, count):
    gid = k + first
    is_first, is_last = gid == 0, gid == count - 1
    before = jnp.where(is_first, k, k - 1)
    after = jnp.where(is_last, k, k + 1)
    stretch = jnp.where(is_first | is_last, F32(count - 1), F32((count - 1) / 2.0))
    return before, after, stretch


def fold(value):
    return jnp.sum(value.reshape(-1, SUBLANES, LANES), axis=0)


def drift_pass(phi, drift, norms, low, high, first, count, own_rows):
    rows = phi.shape[1]
    tiles = phi.shape[2] // LANES

    def body(k, carry):
        before, after, stretch = neighbours_of(k, first, count)
        sums = [jnp.zeros((SUBLANES, LANES), F32), jnp.zeros((SUBLANES, LANES), F32)]

        def use(t, center, total):
            force = total - center * (3.0 + center * center)
            drift[k, :, tile_of(t)] = force
            if t < tiles - 1:
                step = phi[after, 0:own_rows, tile_of(t)] - phi[before, 0:own_rows, tile_of(t)]
                own = force[0:own_rows]
                sums[0] = sums[0] + fold(own * own)
                sums[1] = sums[1] + fold(step * step)

        sum_of_neighbours(lambda t: phi[k, :, tile_of(t)], tiles, rows, use)
        norms[0, pl.ds(k, 1), :] = jnp.sum(sums[0], axis=0, keepdims=True)
        norms[1, pl.ds(k, 1), :] = jnp.sum(sums[1], axis=0, keepdims=True) * (stretch * stretch)
        return carry

    lax.fori_loop(low, high, body, 0)


def speeds_of(norms, speeds):
    force = jnp.sum(norms[0], axis=1, keepdims=True)
    path = jnp.sum(norms[1], axis=1, keepdims=True)
    value = jnp.sqrt(force + EPSILON) / jnp.sqrt(path + EPSILON)
    speeds[...] = jnp.broadcast_to(value, speeds.shape)


def theta_pass(phi, drift, speeds, theta, low, high, first, count):
    tiles = phi.shape[2] // LANES

    def body(k, carry):
        before, after, stretch = neighbours_of(k, first, count)
        scale = speeds[pl.ds(k, 1), :] * stretch
        for t in range(tiles):
            cols = tile_of(t)
            theta[k, :, cols] = scale * (phi[after, :, cols] - phi[before, :, cols]) - drift[k, :, cols]
        return carry

    lax.fori_loop(low, high, body, 0)


def update_pass(phi, speeds, theta, low, high, first, count, store):
    rows = phi.shape[1]
    tiles = phi.shape[2] // LANES

    def body(k, carry):
        before, after, stretch = neighbours_of(k, first, count)
        scale = speeds[pl.ds(k, 1), :] * stretch
        gid = k + first
        inside = (gid > 0) & (gid < count - 1)

        def use(t, center, total):
            cols = tile_of(t)
            value = phi[k, :, cols]
            descent = (
                scale * (theta[after, :, cols] - theta[before, :, cols])
                + total
                - (3.0 * center) * (1.0 + value * value)
            )
            store(k, t, jnp.where(inside, value + TIME_STEP * descent, value))

        sum_of_neighbours(lambda t: theta[k, :, tile_of(t)], tiles, rows, use)
        return carry

    lax.fori_loop(low, high, body, 0)


def start_kernel(*refs, count):
    (keep, recv, near, far, extra_low, extra_high, keep_rows, recv_rows, near_rows, far_rows, extra_rows,
     phi, drift, norms) = refs
    local, rows, _ = keep.shape
    hi, lo = pair_position()
    first = hi * (PAIR * local) - LOW

    def place(source, edge_rows, at, index):
        phi[at, 0:rows, :] = source[index]
        phi[at, rows:, :] = edge_rows[index]

    def body(i, carry):
        place(keep, keep_rows, LOW + lo * local + i, i)
        place(recv, recv_rows, LOW + (1 - lo) * local + i, i)
        low_at, high_at = LOW - local + i, LOW + PAIR * local + i
        place(near, near_rows, jnp.where(lo == 1, low_at, high_at), i)
        place(far, far_rows, jnp.where(lo == 1, high_at, low_at), i)
        return carry

    lax.fori_loop(0, local, body, 0)
    for i in range(LOW - local):

        @pl.when(lo == 0)
        def _():
            phi[i, 0:rows, :] = extra_low[i]

        @pl.when(lo == 1)
        def _():
            phi[i, 0:rows, :] = extra_high[i]

        phi[i, rows:, :] = extra_rows[i]
    norms[...] = jnp.zeros(norms.shape, F32)
    drift_pass(phi, drift, norms, 1, phi.shape[0] - 1, first, count, rows)


def middle_kernel(phi, drift, norms, new_phi, new_drift, new_norms, theta, speeds, *, count, local, rows, done):
    hi, _ = pair_position()
    first = hi * (PAIR * local) - LOW
    window = phi.shape[0]
    speeds_of(norms, speeds)
    theta_pass(phi, drift, speeds, theta, done + 1, window - done - 1, first, count)

    def store(k, t, value):
        new_phi[k, :, tile_of(t)] = value

    update_pass(phi, speeds, theta, done + 2, window - done - 2, first, count, store)
    new_norms[...] = jnp.zeros(new_norms.shape, F32)
    drift_pass(new_phi, new_drift, new_norms, done + 3, window - done - 3, first, count, rows)


def last_kernel(phi, drift, norms, own, down, up, squares, theta, speeds, final, *, count, local, rows, done):
    hi, _ = pair_position()
    first = hi * (PAIR * local) - LOW
    window = phi.shape[0]
    columns = own.shape[2]
    speeds_of(norms, speeds)
    theta_pass(phi, drift, speeds, theta, done + 1, window - done - 1, first, count)

    def store(k, t, value):
        if t < columns // LANES:
            final[k, :, tile_of(t)] = value[0:rows]

    update_pass(phi, speeds, theta, done + 2, window - done - 2, first, count, store)
    position = (
        lax.broadcasted_iota(jnp.int32, squares.shape, 0) * LANES
        + lax.broadcasted_iota(jnp.int32, squares.shape, 1)
    )

    def body(i, total):
        k = LOW + i
        acc = jnp.zeros((SUBLANES, LANES), F32)
        for t in range(columns // LANES):
            value = final[k, :, tile_of(t)]
            own[i, :, tile_of(t)] = value
            diff = value - final[k - 1, :, tile_of(t)]
            acc = acc + fold(diff * diff)
        amount = jnp.sum(jnp.sum(acc, axis=0, keepdims=True), axis=1, keepdims=True)
        return total + jnp.where(position == k + first, amount, 0.0)

    squares[...] = lax.fori_loop(0, PAIR * local, body, jnp.zeros(squares.shape, F32))
    for i in range(REACH + 1):
        down[i] = final[LOW + i]
    for i in range(REACH):
        up[i] = final[LOW + PAIR * local - REACH + i]


def combine_kernel(own_bracket, pair_bracket, own, low, high, squares, keep, send, window, *, count):
    hi, lo = pair_position()
    local = keep.shape[0]
    tiles = own.shape[2] // LANES
    begin = hi * (PAIR * local)
    for i in range(REACH):
        window[i] = low[i]
    for i in range(REACH + 1):
        window[REACH + PAIR * local + i] = high[i]

    def copy(i, carry):
        window[REACH + i] = own[i]
        return carry

    lax.fori_loop(0, PAIR * local, copy, 0)
    position = (
        lax.broadcasted_iota(jnp.int32, squares.shape, 0) * LANES
        + lax.broadcasted_iota(jnp.int32, squares.shape, 1)
    )
    counted = (position >= 1) & (position < count)
    segments = jnp.where(counted, jnp.sqrt(squares[...] + EPSILON), 0.0)

    def total(value):
        return jnp.sum(jnp.sum(value, axis=0, keepdims=True), axis=1, keepdims=True)

    length = total(segments)
    for bracket, part, out in ((own_bracket, lo, keep), (pair_bracket, 1 - lo, send)):

        def body(i, carry):
            b = bracket[i]
            j = begin + part * local + i
            arc = total(jnp.where(position <= b, segments, 0.0))
            segment = total(jnp.where(position == b + 1, segments, 0.0))
            target = length * lax.convert_element_type(j, F32) / F32(count - 1)
            weight = (target - arc) / segment
            at = b - begin + REACH
            for t in range(tiles):
                base = window[at, :, tile_of(t)]
                out[i, :, tile_of(t)] = base + weight * (window[at + 1, :, tile_of(t)] - base)
            return carry

        lax.fori_loop(0, local, body, 0)


def per_device(path, bracket):
    local, rows, columns = path.shape
    devices = lax.axis_size("img")
    count = local * devices
    half = columns // PAIR
    wide = half + LANES
    window = LOW + PAIR * local + HIGH
    if devices & (devices - 1) or local != HIGH or count > SUBLANES * LANES or rows % SUBLANES:
        raise ValueError("unsupported sizes")
    shape = functools.partial(jax.ShapeDtypeStruct, dtype=F32)
    block = shape((local, rows, wide))
    other_bracket = swap_pairs(bracket)
    keep, send = call(pack_kernel, (block, block), operands=1)(path)
    recv = swap_pairs(send)
    ahead = [(i, i + PAIR) for i in range(devices - PAIR)]
    back = [(target, source) for source, target in ahead]
    near = lax.ppermute(keep, "img", [p for p in ahead if p[0] % PAIR == 1] + [p for p in back if p[0] % PAIR == 0])
    far = lax.ppermute(recv, "img", [p for p in ahead if p[0] % PAIR == 0] + [p for p in back if p[0] % PAIR == 1])
    spare = LOW - local
    extra_low = lax.ppermute(keep[-spare:], "img", [p for p in ahead if p[0] % PAIR == 0])
    extra_high = lax.ppermute(recv[-spare:], "img", [p for p in ahead if p[0] % PAIR == 1])
    keep_rows = neighbour_rows(keep)
    late = neighbour_rows(jnp.concatenate([recv, near, far, extra_low + extra_high], axis=0))
    recv_rows, near_rows, far_rows, extra_rows = (
        late[:local], late[local : 2 * local], late[2 * local : 3 * local], late[3 * local :]
    )
    held = shape((window, rows + 2 * EDGE, wide))
    lines = -(-window // SUBLANES) * SUBLANES
    norm_shape = shape((2, lines, LANES))
    phi, drift, norms = call(functools.partial(start_kernel, count=count), (held, held, norm_shape), operands=11)(
        keep, recv, near, far, extra_low, extra_high, keep_rows, recv_rows, near_rows, far_rows, extra_rows
    )
    scratch = [pltpu.VMEM(held.shape, F32), pltpu.VMEM((lines, LANES), F32)]
    for iteration in range(ITERS - 1):
        norms = small_sum(norms, (1,))
        phi, drift, norms = call(
            functools.partial(middle_kernel, count=count, local=local, rows=rows, done=2 * iteration),
            (held, held, norm_shape), scratch=scratch, operands=3,
        )(phi, drift, norms)
    norms = small_sum(norms, (1,))
    half_block = lambda n: shape((n, rows, half))
    own, down, up, squares = call(
        functools.partial(last_kernel, count=count, local=local, rows=rows, done=2 * (ITERS - 1)),
        (half_block(PAIR * local), half_block(REACH + 1), half_block(REACH), shape((SUBLANES, LANES))),
        scratch=scratch + [pltpu.VMEM((window, rows, half), F32)], operands=3,
    )(phi, drift, norms)
    steps = []
    step = 1
    while step < devices:
        steps.append(step)
        step *= 2
    squares = small_sum(squares, steps)
    low = lax.ppermute(up, "img", ahead)
    high = lax.ppermute(down, "img", back)
    mine, theirs = call(
        functools.partial(combine_kernel, count=count), (half_block(local), half_block(local)),
        scratch=[pltpu.VMEM((PAIR * local + 2 * REACH + 1, rows, half), F32)], smem=2, operands=4,
    )(bracket, other_bracket, own, low, high, squares)
    other = swap_pairs(theirs)
    is_low = lax.rem(lax.axis_index("img"), PAIR) == 0
    return jnp.concatenate([jnp.where(is_low, mine, other), jnp.where(is_low, other, mine)], axis=2)


def solution(mesh):
    return jax.shard_map(
        per_device,
        mesh=mesh,
        in_specs=(P(("groups", "img"), "space", None), P(("groups", "img"))),
        out_specs=P(("groups", "img"), "space", None),
        check_vma=False,
    )
```

```python
import functools

import jax
import jax.numpy as jnp
from jax import lax
from jax.experimental import pallas as pl
from jax.experimental.pallas import tpu as pltpu
from jax.sharding import PartitionSpec as P


REACH = 2
ITERS = 2
TIME_STEP = 0.002
EPSILON = 1e-06

LANES = 128
SUBLANES = 8
PAIR = 2
LOW = 2 * ITERS + REACH
HIGH = 2 * ITERS + REACH + 1
FAR = 3
EDGE = 2 * ITERS
CHUNKS = (0, 1, 2, 3)
VMEM_LIMIT = 12 * 1024 * 1024

F32 = jnp.float32


def call(kernel, out_shapes, scratch=(), smem=0, operands=0):
    specs = [pl.BlockSpec(memory_space=pltpu.SMEM)] * smem
    specs += [pl.BlockSpec(memory_space=pltpu.VMEM)] * operands
    return pl.pallas_call(
        kernel,
        out_shape=out_shapes,
        in_specs=specs,
        out_specs=jax.tree.map(lambda _: pl.BlockSpec(memory_space=pltpu.VMEM), out_shapes),
        scratch_shapes=list(scratch),
        compiler_params=pltpu.CompilerParams(vmem_limit_bytes=VMEM_LIMIT),
    )


def pair_position():
    index = lax.axis_index("img")
    return lax.div(index, PAIR), lax.rem(index, PAIR)


def swap_pairs(value):
    count = lax.axis_size("img")
    return lax.ppermute(value, "img", [(i, i ^ 1) for i in range(count)])


def small_sum(value, steps):
    size = lax.axis_size("space")
    if size & (size - 1) == 0:
        step = 1
        while step < size:
            value = value + lax.ppermute(value, "space", [(i, i ^ step) for i in range(size)])
            step *= 2
    else:
        value = lax.psum(value, "space")
    count = lax.axis_size("img")
    for step in steps:
        value = value + lax.ppermute(value, "img", [(i, i ^ step) for i in range(count)])
    return value


def neighbour_rows(blocks):
    size = lax.axis_size("space")
    top = jnp.concatenate([block[:, :EDGE] for block in blocks], axis=0)
    bottom = jnp.concatenate([block[:, -EDGE:] for block in blocks], axis=0)
    if size == 1:
        return jnp.concatenate([top, bottom], axis=1)
    if size == 2:
        return lax.ppermute(jnp.concatenate([top, bottom], axis=1), "space", [(0, 1), (1, 0)])
    after = lax.ppermute(top, "space", [(i, (i - 1) % size) for i in range(size)])
    before = lax.ppermute(bottom, "space", [(i, (i + 1) % size) for i in range(size)])
    return jnp.concatenate([after, before], axis=1)


def pack_kernel(x_ref, keep_ref, send_ref):
    _, lo = pair_position()
    columns = x_ref.shape[2]
    half = columns // PAIR
    lane = lax.broadcasted_iota(jnp.int32, (x_ref.shape[1], LANES), 1)

    local = x_ref.shape[0]

    def body(q, carry):
        k = jnp.where(lo == 0, q, local - 1 - q)
        for ref, part in ((keep_ref, lo), (send_ref, 1 - lo)):
            begin = pl.multiple_of(part * half, LANES)
            right = pl.multiple_of((1 - part) * half, LANES)
            left = pl.multiple_of((1 - part) * half + half - LANES, LANES)
            ref[q, :, 0:half] = x_ref[k, :, pl.ds(begin, half)]
            ref[q, :, half:] = jnp.where(
                lane < LANES // 2, x_ref[k, :, pl.ds(right, LANES)], x_ref[k, :, pl.ds(left, LANES)]
            )
        return carry

    lax.fori_loop(0, local, body, 0)


def sum_of_neighbours(load, tiles, rows, use):
    lane = lax.broadcasted_iota(jnp.int32, (rows, LANES), 1)
    is_first, is_last = lane == 0, lane == LANES - 1
    center = load(0)
    from_left = pltpu.roll(load(tiles - 1), 1, 1)
    to_left = pltpu.roll(center, LANES - 1, 1)
    for t in range(tiles):
        following = load((t + 1) % tiles)
        shifted = pltpu.roll(center, 1, 1)
        next_to_left = pltpu.roll(following, LANES - 1, 1)
        west = jnp.where(is_first, from_left, shifted)
        east = jnp.where(is_last, next_to_left, to_left)
        north = pltpu.roll(center, 1, 0)
        south = pltpu.roll(center, rows - 1, 0)
        use(t, center, (north + south) + (west + east))
        center, from_left, to_left = following, shifted, next_to_left


def tile_of(t):
    return slice(t * LANES, (t + 1) * LANES)


def neighbours_of(k, first, count):
    gid = k + first
    is_first, is_last = gid == 0, gid == count - 1
    before = jnp.where(is_first, k, k - 1)
    after = jnp.where(is_last, k, k + 1)
    stretch = jnp.where(is_first | is_last, F32(count - 1), F32((count - 1) / 2.0))
    return before, after, stretch


def fold(value):
    return jnp.sum(value.reshape(-1, SUBLANES, LANES), axis=0)


def drift_pass(phi, drift, norms, low, high, first, count, own_rows):
    rows = phi.shape[1]
    tiles = phi.shape[2] // LANES

    def body(k, carry):
        before, after, stretch = neighbours_of(k, first, count)
        sums = [jnp.zeros((SUBLANES, LANES), F32), jnp.zeros((SUBLANES, LANES), F32)]

        def use(t, center, total):
            force = total - center * (3.0 + center * center)
            drift[k, :, tile_of(t)] = force
            if t < tiles - 1:
                step = phi[after, 0:own_rows, tile_of(t)] - phi[before, 0:own_rows, tile_of(t)]
                own = force[0:own_rows]
                sums[0] = sums[0] + fold(own * own)
                sums[1] = sums[1] + fold(step * step)

        sum_of_neighbours(lambda t: phi[k, :, tile_of(t)], tiles, rows, use)
        norms[0, pl.ds(k, 1), :] = jnp.sum(sums[0], axis=0, keepdims=True)
        norms[1, pl.ds(k, 1), :] = jnp.sum(sums[1], axis=0, keepdims=True) * (stretch * stretch)
        return carry

    lax.fori_loop(low, high, body, 0)


def speeds_of(norms, speeds):
    force = jnp.sum(norms[0], axis=1, keepdims=True)
    path = jnp.sum(norms[1], axis=1, keepdims=True)
    value = jnp.sqrt(force + EPSILON) / jnp.sqrt(path + EPSILON)
    speeds[...] = jnp.broadcast_to(value, speeds.shape)


def theta_pass(phi, drift, speeds, theta, low, high, first, count):
    tiles = phi.shape[2] // LANES

    def body(k, carry):
        before, after, stretch = neighbours_of(k, first, count)
        scale = speeds[pl.ds(k, 1), :] * stretch
        for t in range(tiles):
            cols = tile_of(t)
            theta[k, :, cols] = scale * (phi[after, :, cols] - phi[before, :, cols]) - drift[k, :, cols]
        return carry

    lax.fori_loop(low, high, body, 0)


def update_pass(phi, speeds, theta, low, high, first, count, store):
    rows = phi.shape[1]
    tiles = phi.shape[2] // LANES

    def body(k, carry):
        before, after, stretch = neighbours_of(k, first, count)
        scale = speeds[pl.ds(k, 1), :] * stretch
        gid = k + first
        inside = (gid > 0) & (gid < count - 1)

        def use(t, center, total):
            cols = tile_of(t)
            value = phi[k, :, cols]
            descent = (
                scale * (theta[after, :, cols] - theta[before, :, cols])
                + total
                - (3.0 * center) * (1.0 + value * value)
            )
            store(k, t, jnp.where(inside, value + TIME_STEP * descent, value))

        sum_of_neighbours(lambda t: theta[k, :, tile_of(t)], tiles, rows, use)
        return carry

    lax.fori_loop(low, high, body, 0)


def start_kernel(*refs, count, splits):
    refs = list(refs)
    pick = lambda n: [refs.pop(0) for _ in range(n)]
    keep, near_early, far_early = pick(3)
    recv, near_late = pick(len(splits)), pick(len(splits))
    far_late, far_last = pick(2)
    rows_early, rows_late, phi, drift, norms = pick(5)
    local, rows, _ = keep.shape
    hi, lo = pair_position()
    first = hi * (PAIR * local) - LOW
    top = LOW + PAIR * local

    def place(at, image, edge_rows):
        phi[at, 0:rows, :] = image
        phi[at, rows:, :] = edge_rows

    def own_at(part, q):
        return LOW + part * local + jnp.where(part == 0, q, local - 1 - q)

    for q in range(local):
        chunk = max(c for c in range(len(splits)) if splits[c] <= q)
        at = q - splits[chunk]
        place(own_at(lo, q), keep[q], rows_early[q])
        place(own_at(1 - lo, q), recv[chunk][at], rows_late[q])
        low_at, high_at = LOW - 1 - q, top + q
        place(jnp.where(lo == 1, low_at, high_at), near_early[q], rows_early[local + q])
        place(jnp.where(lo == 1, high_at, low_at), near_late[chunk][at], rows_late[local + q])
    for i in range(FAR):
        low_at, high_at = LOW - 1 - local - i, top + local + i
        late = far_late.at[1 - i] if i < 2 else far_last.at[0]
        late_rows = rows_late.at[2 * local + i]
        early, early_rows = far_early.at[FAR - 1 - i], rows_early.at[2 * local + i]

        @pl.when(lo == 1)
        def _():
            if high_at < phi.shape[0]:
                place(high_at, early[...], early_rows[...])
            if low_at >= 0:
                place(low_at, late[...], late_rows[...])

        @pl.when(lo == 0)
        def _():
            if high_at < phi.shape[0]:
                place(high_at, late[...], late_rows[...])
            if low_at >= 0:
                place(low_at, early[...], early_rows[...])

    norms[...] = jnp.zeros(norms.shape, F32)
    drift_pass(phi, drift, norms, 1, phi.shape[0] - 1, first, count, rows)


def middle_kernel(phi, drift, norms, new_phi, new_drift, new_norms, theta, speeds, *, count, local, rows, done):
    hi, _ = pair_position()
    first = hi * (PAIR * local) - LOW
    window = phi.shape[0]
    speeds_of(norms, speeds)
    theta_pass(phi, drift, speeds, theta, done + 1, window - done - 1, first, count)

    def store(k, t, value):
        new_phi[k, :, tile_of(t)] = value

    update_pass(phi, speeds, theta, done + 2, window - done - 2, first, count, store)
    new_norms[...] = jnp.zeros(new_norms.shape, F32)
    drift_pass(new_phi, new_drift, new_norms, done + 3, window - done - 3, first, count, rows)


def last_kernel(phi, drift, norms, final, squares, theta, speeds, *, count, local, rows, done):
    hi, _ = pair_position()
    first = hi * (PAIR * local) - LOW
    window = phi.shape[0]
    tiles = final.shape[2] // LANES
    shift = LOW - REACH
    speeds_of(norms, speeds)
    theta_pass(phi, drift, speeds, theta, done + 1, window - done - 1, first, count)

    def store(k, t, value):
        if t < tiles:
            final[k - shift, :, tile_of(t)] = value[0:rows]

    update_pass(phi, speeds, theta, shift, shift + final.shape[0], first, count, store)
    position = (
        lax.broadcasted_iota(jnp.int32, squares.shape, 0) * LANES
        + lax.broadcasted_iota(jnp.int32, squares.shape, 1)
    )

    def body(i, total):
        k = REACH + i
        acc = jnp.zeros((SUBLANES, LANES), F32)
        for t in range(tiles):
            diff = final[k, :, tile_of(t)] - final[k - 1, :, tile_of(t)]
            acc = acc + fold(diff * diff)
        amount = jnp.sum(jnp.sum(acc, axis=0, keepdims=True), axis=1, keepdims=True)
        return total + jnp.where(position == LOW + i + first, amount, 0.0)

    squares[...] = lax.fori_loop(0, PAIR * local, body, jnp.zeros(squares.shape, F32))


def combine_kernel(bracket, window, squares, out, *, count, own):
    hi, lo = pair_position()
    part = lo if own else 1 - lo
    local = out.shape[0]
    tiles = out.shape[2] // LANES
    begin = hi * (PAIR * local)
    position = (
        lax.broadcasted_iota(jnp.int32, squares.shape, 0) * LANES
        + lax.broadcasted_iota(jnp.int32, squares.shape, 1)
    )
    counted = (position >= 1) & (position < count)
    segments = jnp.where(counted, jnp.sqrt(squares[...] + EPSILON), 0.0)

    def total(value):
        return jnp.sum(jnp.sum(value, axis=0, keepdims=True), axis=1, keepdims=True)

    length = total(segments)
    weights = []
    for i in range(local):
        b = bracket[i]
        j = begin + part * local + i
        arc = total(jnp.where(position <= b, segments, 0.0))
        segment = total(jnp.where(position == b + 1, segments, 0.0))
        target = length * lax.convert_element_type(j, F32) / F32(count - 1)
        weights.append((target - arc) / segment)
    for i in range(local):
        at = bracket[i] - begin + REACH
        for t in range(tiles):
            base = window[at, :, tile_of(t)]
            out[i, :, tile_of(t)] = base + weights[i] * (window[at + 1, :, tile_of(t)] - base)


def per_device(path, bracket):
    local, rows, columns = path.shape
    devices = lax.axis_size("img")
    count = local * devices
    half = columns // PAIR
    wide = half + LANES
    window = LOW + PAIR * local + HIGH
    if devices & (devices - 1) or local != 2 * ITERS or count > SUBLANES * LANES or rows % SUBLANES:
        raise ValueError("unsupported sizes")
    shape = functools.partial(jax.ShapeDtypeStruct, dtype=F32)
    block = shape((local, rows, wide))
    ahead = [(i, i + PAIR) for i in range(devices - PAIR)]
    back = [(target, source) for source, target in ahead]
    move = lambda value, up, down: lax.ppermute(
        value, "img",
        [p for p in ahead if p[0] % PAIR in up] + [p for p in back if p[0] % PAIR in down],
    )
    other_bracket = swap_pairs(bracket)
    keep, send = call(pack_kernel, (block, block), operands=1)(path)
    splits = CHUNKS
    ends = splits[1:] + (local,)
    recv = [swap_pairs(send[a:b]) for a, b in zip(splits, ends)]
    near_early = move(keep, (1,), (0,))
    far_early = move(keep[local - FAR :], (0,), (1,))
    near_late = [move(value, (0,), (1,)) for value in recv]
    images = jnp.concatenate(recv, axis=0)
    far_last = move(images[local - FAR : local - 2], (), (0,))
    far_late = move(images[local - 2 :], (1,), (0,))
    flip = lambda value: jnp.concatenate([value[i : i + 1] for i in reversed(range(value.shape[0]))], axis=0)
    rows_early = neighbour_rows([keep, near_early, flip(far_early)])
    rows_late = neighbour_rows(recv + near_late + [flip(far_late), far_last])
    held = shape((window, rows + 2 * EDGE, wide))
    lines = -(-window // SUBLANES) * SUBLANES
    norm_shape = shape((2, lines, LANES))
    operands = [keep, near_early, far_early] + recv + near_late + [far_late, far_last, rows_early, rows_late]
    phi, drift, norms = call(
        functools.partial(start_kernel, count=count, splits=splits), (held, held, norm_shape),
        operands=len(operands),
    )(*operands)
    other_bracket, norms = lax.optimization_barrier((other_bracket, norms))
    scratch = [pltpu.VMEM(held.shape, F32), pltpu.VMEM((lines, LANES), F32)]
    for iteration in range(ITERS - 1):
        norms = small_sum(norms, (1,))
        phi, drift, norms = call(
            functools.partial(middle_kernel, count=count, local=local, rows=rows, done=2 * iteration),
            (held, held, norm_shape), scratch=scratch, operands=3,
        )(phi, drift, norms)
    norms = small_sum(norms, (1,))
    final, squares = call(
        functools.partial(last_kernel, count=count, local=local, rows=rows, done=2 * (ITERS - 1)),
        (shape((PAIR * local + 2 * REACH + 1, rows, half)), shape((SUBLANES, LANES))),
        scratch=scratch, operands=3,
    )(phi, drift, norms)
    steps = []
    step = 1
    while step < devices:
        steps.append(step)
        step *= 2
    squares = small_sum(squares, steps)
    combine = lambda chosen, own: call(
        functools.partial(combine_kernel, count=count, own=own), shape((local, rows, half)), smem=1, operands=2
    )(chosen, final, squares)
    other = swap_pairs(combine(other_bracket, False))
    mine = combine(bracket, True)
    is_low = lax.rem(lax.axis_index("img"), PAIR) == 0
    return jnp.concatenate([jnp.where(is_low, mine, other), jnp.where(is_low, other, mine)], axis=2)


def solution(mesh):
    return jax.shard_map(
        per_device,
        mesh=mesh,
        in_specs=(P(("groups", "img"), "space", None), P(("groups", "img"))),
        out_specs=P(("groups", "img"), "space", None),
        check_vma=False,
    )
```

```python
import functools

import jax
import jax.numpy as jnp
from jax import lax
from jax.experimental import pallas as pl
from jax.experimental.pallas import tpu as pltpu
from jax.sharding import PartitionSpec as P


REACH = 2
ITERS = 2
TIME_STEP = 0.002
EPSILON = 1e-06

LANES = 128
SUBLANES = 8
PAIR = 2
LOW = 2 * ITERS + REACH
HIGH = 2 * ITERS + REACH + 1
FAR = 3
EDGE = 2 * ITERS
CHUNKS = (0, 3)
VMEM_LIMIT = 12 * 1024 * 1024

F32 = jnp.float32


def call(kernel, out_shapes, scratch=(), smem=0, operands=0):
    specs = [pl.BlockSpec(memory_space=pltpu.SMEM)] * smem
    specs += [pl.BlockSpec(memory_space=pltpu.VMEM)] * operands
    return pl.pallas_call(
        kernel,
        out_shape=out_shapes,
        in_specs=specs,
        out_specs=jax.tree.map(lambda _: pl.BlockSpec(memory_space=pltpu.VMEM), out_shapes),
        scratch_shapes=list(scratch),
        compiler_params=pltpu.CompilerParams(vmem_limit_bytes=VMEM_LIMIT),
    )


def pair_position():
    index = lax.axis_index("img")
    return lax.div(index, PAIR), lax.rem(index, PAIR)


def swap_pairs(value):
    count = lax.axis_size("img")
    return lax.ppermute(value, "img", [(i, i ^ 1) for i in range(count)])


def small_sum(value, steps):
    size = lax.axis_size("space")
    if size & (size - 1) == 0:
        step = 1
        while step < size:
            value = value + lax.ppermute(value, "space", [(i, i ^ step) for i in range(size)])
            step *= 2
    else:
        value = lax.psum(value, "space")
    count = lax.axis_size("img")
    for step in steps:
        value = value + lax.ppermute(value, "img", [(i, i ^ step) for i in range(count)])
    return value


def neighbour_rows(blocks):
    size = lax.axis_size("space")
    top = jnp.concatenate([block[:, :EDGE] for block in blocks], axis=0)
    bottom = jnp.concatenate([block[:, -EDGE:] for block in blocks], axis=0)
    if size == 1:
        return jnp.concatenate([top, bottom], axis=1)
    if size == 2:
        return lax.ppermute(jnp.concatenate([top, bottom], axis=1), "space", [(0, 1), (1, 0)])
    after = lax.ppermute(top, "space", [(i, (i - 1) % size) for i in range(size)])
    before = lax.ppermute(bottom, "space", [(i, (i + 1) % size) for i in range(size)])
    return jnp.concatenate([after, before], axis=1)


def pack_kernel(x_ref, keep_ref, send_ref):
    _, lo = pair_position()
    columns = x_ref.shape[2]
    half = columns // PAIR
    lane = lax.broadcasted_iota(jnp.int32, (x_ref.shape[1], LANES), 1)

    local = x_ref.shape[0]

    def body(q, carry):
        k = jnp.where(lo == 0, q, local - 1 - q)
        for ref, part in ((keep_ref, lo), (send_ref, 1 - lo)):
            begin = pl.multiple_of(part * half, LANES)
            right = pl.multiple_of((1 - part) * half, LANES)
            left = pl.multiple_of((1 - part) * half + half - LANES, LANES)
            ref[q, :, 0:half] = x_ref[k, :, pl.ds(begin, half)]
            ref[q, :, half:] = jnp.where(
                lane < LANES // 2, x_ref[k, :, pl.ds(right, LANES)], x_ref[k, :, pl.ds(left, LANES)]
            )
        return carry

    lax.fori_loop(0, local, body, 0)


def sum_of_neighbours(load, tiles, rows, use):
    lane = lax.broadcasted_iota(jnp.int32, (rows, LANES), 1)
    is_first, is_last = lane == 0, lane == LANES - 1
    center = load(0)
    from_left = pltpu.roll(load(tiles - 1), 1, 1)
    to_left = pltpu.roll(center, LANES - 1, 1)
    for t in range(tiles):
        following = load((t + 1) % tiles)
        shifted = pltpu.roll(center, 1, 1)
        next_to_left = pltpu.roll(following, LANES - 1, 1)
        west = jnp.where(is_first, from_left, shifted)
        east = jnp.where(is_last, next_to_left, to_left)
        north = pltpu.roll(center, 1, 0)
        south = pltpu.roll(center, rows - 1, 0)
        use(t, center, (north + south) + (west + east))
        center, from_left, to_left = following, shifted, next_to_left


def tile_of(t):
    return slice(t * LANES, (t + 1) * LANES)


def neighbours_of(k, first, count):
    gid = k + first
    is_first, is_last = gid == 0, gid == count - 1
    before = jnp.where(is_first, k, k - 1)
    after = jnp.where(is_last, k, k + 1)
    stretch = jnp.where(is_first | is_last, F32(count - 1), F32((count - 1) / 2.0))
    return before, after, stretch


def fold(value):
    return jnp.sum(value.reshape(-1, SUBLANES, LANES), axis=0)


def drift_pass(phi, drift, norms, low, high, first, count, own_rows):
    rows = phi.shape[1]
    tiles = phi.shape[2] // LANES

    def body(k, carry):
        before, after, stretch = neighbours_of(k, first, count)
        sums = [jnp.zeros((SUBLANES, LANES), F32), jnp.zeros((SUBLANES, LANES), F32)]

        def use(t, center, total):
            force = total - center * (3.0 + center * center)
            drift[k, :, tile_of(t)] = force
            if t < tiles - 1:
                step = phi[after, 0:own_rows, tile_of(t)] - phi[before, 0:own_rows, tile_of(t)]
                own = force[0:own_rows]
                sums[0] = sums[0] + fold(own * own)
                sums[1] = sums[1] + fold(step * step)

        sum_of_neighbours(lambda t: phi[k, :, tile_of(t)], tiles, rows, use)
        norms[0, pl.ds(k, 1), :] = jnp.sum(sums[0], axis=0, keepdims=True)
        norms[1, pl.ds(k, 1), :] = jnp.sum(sums[1], axis=0, keepdims=True) * (stretch * stretch)
        return carry

    lax.fori_loop(low, high, body, 0)


def speeds_of(norms, speeds):
    force = jnp.sum(norms[0], axis=1, keepdims=True)
    path = jnp.sum(norms[1], axis=1, keepdims=True)
    value = jnp.sqrt(force + EPSILON) / jnp.sqrt(path + EPSILON)
    speeds[...] = jnp.broadcast_to(value, speeds.shape)


def theta_pass(phi, drift, speeds, theta, low, high, first, count):
    tiles = phi.shape[2] // LANES

    def body(k, carry):
        before, after, stretch = neighbours_of(k, first, count)
        scale = speeds[pl.ds(k, 1), :] * stretch
        for t in range(tiles):
            cols = tile_of(t)
            theta[k, :, cols] = scale * (phi[after, :, cols] - phi[before, :, cols]) - drift[k, :, cols]
        return carry

    lax.fori_loop(low, high, body, 0)


def update_pass(phi, speeds, theta, low, high, first, count, store):
    rows = phi.shape[1]
    tiles = phi.shape[2] // LANES

    def body(k, carry):
        before, after, stretch = neighbours_of(k, first, count)
        scale = speeds[pl.ds(k, 1), :] * stretch
        gid = k + first
        inside = (gid > 0) & (gid < count - 1)

        def use(t, center, total):
            cols = tile_of(t)
            value = phi[k, :, cols]
            descent = (
                scale * (theta[after, :, cols] - theta[before, :, cols])
                + total
                - (3.0 * center) * (1.0 + value * value)
            )
            store(k, t, jnp.where(inside, value + TIME_STEP * descent, value))

        sum_of_neighbours(lambda t: theta[k, :, tile_of(t)], tiles, rows, use)
        return carry

    lax.fori_loop(low, high, body, 0)


def start_kernel(*refs, count, splits):
    refs = list(refs)
    pick = lambda n: [refs.pop(0) for _ in range(n)]
    keep, near_early, far_early = pick(3)
    recv, near_late = pick(len(splits)), pick(len(splits))
    far_late = pick(len(splits))
    rows_early, rows_late, phi, drift, norms = pick(5)
    local, rows, _ = keep.shape
    hi, lo = pair_position()
    first = hi * (PAIR * local) - LOW
    top = LOW + PAIR * local

    def place(at, image, edge_rows):
        phi[at, 0:rows, :] = image
        phi[at, rows:, :] = edge_rows

    def chunk_of(q):
        return max(c for c in range(len(splits)) if splits[c] <= q)

    def own_at(part, q):
        return LOW + part * local + jnp.where(part == 0, q, local - 1 - q)

    for q in range(local):
        chunk = chunk_of(q)
        at = q - splits[chunk]
        place(own_at(lo, q), keep[q], rows_early[q])
        place(own_at(1 - lo, q), recv[chunk][at], rows_late[q])
        low_at, high_at = LOW - 1 - q, top + q
        place(jnp.where(lo == 1, low_at, high_at), near_early[q], rows_early[local + q])
        place(jnp.where(lo == 1, high_at, low_at), near_late[chunk][at], rows_late[local + q])
    for i in range(FAR):
        low_at, high_at = LOW - 1 - local - i, top + local + i
        q = local - 1 - i
        late = far_late[chunk_of(q)].at[q - max(splits[chunk_of(q)], local - FAR)]
        late_rows = rows_late.at[2 * local + i]
        early, early_rows = far_early.at[FAR - 1 - i], rows_early.at[2 * local + i]

        @pl.when(lo == 1)
        def _():
            if high_at < phi.shape[0]:
                place(high_at, early[...], early_rows[...])
            if low_at >= 0:
                place(low_at, late[...], late_rows[...])

        @pl.when(lo == 0)
        def _():
            if high_at < phi.shape[0]:
                place(high_at, late[...], late_rows[...])
            if low_at >= 0:
                place(low_at, early[...], early_rows[...])

    norms[...] = jnp.zeros(norms.shape, F32)
    drift_pass(phi, drift, norms, 1, phi.shape[0] - 1, first, count, rows)


def middle_kernel(phi, drift, norms, new_phi, new_drift, new_norms, theta, speeds, *, count, local, rows, done):
    hi, _ = pair_position()
    first = hi * (PAIR * local) - LOW
    window = phi.shape[0]
    speeds_of(norms, speeds)
    theta_pass(phi, drift, speeds, theta, done + 1, window - done - 1, first, count)

    def store(k, t, value):
        new_phi[k, :, tile_of(t)] = value

    update_pass(phi, speeds, theta, done + 2, window - done - 2, first, count, store)
    new_norms[...] = jnp.zeros(new_norms.shape, F32)
    drift_pass(new_phi, new_drift, new_norms, done + 3, window - done - 3, first, count, rows)


def last_kernel(phi, drift, norms, final, squares, theta, speeds, *, count, local, rows, done):
    hi, _ = pair_position()
    first = hi * (PAIR * local) - LOW
    window = phi.shape[0]
    tiles = final.shape[2] // LANES
    shift = LOW - REACH
    speeds_of(norms, speeds)
    theta_pass(phi, drift, speeds, theta, done + 1, window - done - 1, first, count)

    def store(k, t, value):
        if t < tiles:
            final[k - shift, :, tile_of(t)] = value[0:rows]

    update_pass(phi, speeds, theta, shift, shift + final.shape[0], first, count, store)
    position = (
        lax.broadcasted_iota(jnp.int32, squares.shape, 0) * LANES
        + lax.broadcasted_iota(jnp.int32, squares.shape, 1)
    )

    def body(i, total):
        k = REACH + i
        acc = jnp.zeros((SUBLANES, LANES), F32)
        for t in range(tiles):
            diff = final[k, :, tile_of(t)] - final[k - 1, :, tile_of(t)]
            acc = acc + fold(diff * diff)
        amount = jnp.sum(jnp.sum(acc, axis=0, keepdims=True), axis=1, keepdims=True)
        return total + jnp.where(position == LOW + i + first, amount, 0.0)

    squares[...] = lax.fori_loop(0, PAIR * local, body, jnp.zeros(squares.shape, F32))


def combine_kernel(bracket, window, squares, out, *scratch, count, own):
    hi, lo = pair_position()
    part = lo if own else 1 - lo
    whole, out = out, scratch[0] if own else out
    local, _, half = out.shape
    tiles = half // LANES
    begin = hi * (PAIR * local)
    position = (
        lax.broadcasted_iota(jnp.int32, squares.shape, 0) * LANES
        + lax.broadcasted_iota(jnp.int32, squares.shape, 1)
    )
    counted = (position >= 1) & (position < count)
    segments = jnp.where(counted, jnp.sqrt(squares[...] + EPSILON), 0.0)

    def total(value):
        return jnp.sum(jnp.sum(value, axis=0, keepdims=True), axis=1, keepdims=True)

    length = total(segments)
    weights = []
    for i in range(local):
        b = bracket[i]
        j = begin + part * local + i
        arc = total(jnp.where(position <= b, segments, 0.0))
        segment = total(jnp.where(position == b + 1, segments, 0.0))
        target = length * lax.convert_element_type(j, F32) / F32(count - 1)
        weights.append((target - arc) / segment)
    for i in range(local):
        at = bracket[i] - begin + REACH
        for t in range(tiles):
            base = window[at, :, tile_of(t)]
            out[i, :, tile_of(t)] = base + weights[i] * (window[at + 1, :, tile_of(t)] - base)
    if own:
        copy_half(out, whole, lo, scratch[1])


def copy_half(half_ref, whole, part, sem):
    half = half_ref.shape[2]
    copy = pltpu.make_async_copy(half_ref, whole.at[:, :, pl.ds(pl.multiple_of(part * half, LANES), half)], sem)
    copy.start()
    copy.wait()


def finish_kernel(whole_in, other, whole, sem):
    _, lo = pair_position()
    copy_half(other, whole, 1 - lo, sem)


def per_device(path, bracket):
    local, rows, columns = path.shape
    devices = lax.axis_size("img")
    count = local * devices
    half = columns // PAIR
    wide = half + LANES
    window = LOW + PAIR * local + HIGH
    if devices & (devices - 1) or local != 2 * ITERS or count > SUBLANES * LANES or rows % SUBLANES:
        raise ValueError("unsupported sizes")
    shape = functools.partial(jax.ShapeDtypeStruct, dtype=F32)
    block = shape((local, rows, wide))
    ahead = [(i, i + PAIR) for i in range(devices - PAIR)]
    back = [(target, source) for source, target in ahead]
    move = lambda value, up, down: lax.ppermute(
        value, "img",
        [p for p in ahead if p[0] % PAIR in up] + [p for p in back if p[0] % PAIR in down],
    )
    other_bracket = swap_pairs(bracket)
    keep, send = call(pack_kernel, (block, block), operands=1)(path)
    splits = CHUNKS
    ends = splits[1:] + (local,)
    recv = [swap_pairs(send[a:b]) for a, b in zip(splits, ends)]
    near_early = move(keep, (1,), (0,))
    far_early = move(keep[local - FAR :], (0,), (1,))
    near_late = [move(value, (0,), (1,)) for value in recv]
    far_late = [
        move(value[max(0, local - FAR - a) :], (1,), (0,))
        for a, value in zip(splits, recv)
    ]
    flip = lambda value: jnp.concatenate([value[i : i + 1] for i in reversed(range(value.shape[0]))], axis=0)
    rows_early = neighbour_rows([keep, near_early, flip(far_early)])
    rows_late = neighbour_rows(recv + near_late + [flip(value) for value in reversed(far_late)])
    held = shape((window, rows + 2 * EDGE, wide))
    lines = -(-window // SUBLANES) * SUBLANES
    norm_shape = shape((2, lines, LANES))
    operands = [keep, near_early, far_early] + recv + near_late + far_late + [rows_early, rows_late]
    phi, drift, norms = call(
        functools.partial(start_kernel, count=count, splits=splits), (held, held, norm_shape),
        operands=len(operands),
    )(*operands)
    other_bracket, norms = lax.optimization_barrier((other_bracket, norms))
    scratch = [pltpu.VMEM(held.shape, F32), pltpu.VMEM((lines, LANES), F32)]
    for iteration in range(ITERS - 1):
        norms = small_sum(norms, (1,))
        phi, drift, norms = call(
            functools.partial(middle_kernel, count=count, local=local, rows=rows, done=2 * iteration),
            (held, held, norm_shape), scratch=scratch, operands=3,
        )(phi, drift, norms)
    norms = small_sum(norms, (1,))
    final, squares = call(
        functools.partial(last_kernel, count=count, local=local, rows=rows, done=2 * (ITERS - 1)),
        (shape((PAIR * local + 2 * REACH + 1, rows, half)), shape((SUBLANES, LANES))),
        scratch=scratch, operands=3,
    )(phi, drift, norms)
    steps = []
    step = 1
    while step < devices:
        steps.append(step)
        step *= 2
    squares = small_sum(squares, steps)
    half_block = (local, rows, half)
    whole = shape((local, rows, columns))
    in_smem, in_vmem, in_hbm = (pl.BlockSpec(memory_space=m) for m in (pltpu.SMEM, pltpu.VMEM, pl.ANY))
    other = swap_pairs(
        call(functools.partial(combine_kernel, count=count, own=False), shape(half_block), smem=1, operands=2)(
            other_bracket, final, squares
        )
    )
    mine = pl.pallas_call(
        functools.partial(combine_kernel, count=count, own=True),
        out_shape=whole,
        in_specs=[in_smem, in_vmem, in_vmem],
        out_specs=in_hbm,
        scratch_shapes=[pltpu.VMEM(half_block, F32), pltpu.SemaphoreType.DMA],
        compiler_params=pltpu.CompilerParams(vmem_limit_bytes=VMEM_LIMIT),
    )(bracket, final, squares)
    return pl.pallas_call(
        finish_kernel,
        out_shape=whole,
        in_specs=[in_hbm, in_vmem],
        out_specs=in_hbm,
        scratch_shapes=[pltpu.SemaphoreType.DMA],
        input_output_aliases={0: 0},
        compiler_params=pltpu.CompilerParams(vmem_limit_bytes=VMEM_LIMIT),
    )(mine, other)


def solution(mesh):
    return jax.shard_map(
        per_device,
        mesh=mesh,
        in_specs=(P(("groups", "img"), "space", None), P(("groups", "img"))),
        out_specs=P(("groups", "img"), "space", None),
        check_vma=False,
    )
```

```python
import functools

import jax
import jax.numpy as jnp
from jax import lax
from jax.experimental import pallas as pl
from jax.experimental.pallas import tpu as pltpu
from jax.sharding import PartitionSpec as P


REACH = 2
ITERS = 2
TIME_STEP = 0.002
EPSILON = 1e-06

LANES = 128
SUBLANES = 8
PAIR = 2
LOW = 2 * ITERS + REACH
HIGH = 2 * ITERS + REACH + 1
FAR = 3
EDGE = 2 * ITERS
CHUNKS = (0, 1, 3)
VMEM_LIMIT = 12 * 1024 * 1024

F32 = jnp.float32


def call(kernel, out_shapes, scratch=(), smem=0, operands=0, aliases=None):
    specs = [pl.BlockSpec(memory_space=pltpu.SMEM)] * smem
    specs += [pl.BlockSpec(memory_space=pltpu.VMEM)] * operands
    return pl.pallas_call(
        kernel,
        out_shape=out_shapes,
        in_specs=specs,
        out_specs=jax.tree.map(lambda _: pl.BlockSpec(memory_space=pltpu.VMEM), out_shapes),
        scratch_shapes=list(scratch),
        input_output_aliases=aliases or {},
        compiler_params=pltpu.CompilerParams(vmem_limit_bytes=VMEM_LIMIT),
    )


def pair_position():
    index = lax.axis_index("img")
    return lax.div(index, PAIR), lax.rem(index, PAIR)


def swap_pairs(value):
    count = lax.axis_size("img")
    return lax.ppermute(value, "img", [(i, i ^ 1) for i in range(count)])


def small_sum(value, steps):
    size = lax.axis_size("space")
    if size & (size - 1) == 0:
        step = 1
        while step < size:
            value = value + lax.ppermute(value, "space", [(i, i ^ step) for i in range(size)])
            step *= 2
    else:
        value = lax.psum(value, "space")
    count = lax.axis_size("img")
    for step in steps:
        value = value + lax.ppermute(value, "img", [(i, i ^ step) for i in range(count)])
    return value


def pick_kernel(*refs):
    *blocks, picked = refs
    at = 0
    for block in blocks:
        for i in range(block.shape[0]):
            picked[at, 0:EDGE, :] = block[i, 0:EDGE, :]
            picked[at, EDGE:, :] = block[i, block.shape[1] - EDGE :, :]
            at += 1


def neighbour_rows(blocks):
    size = lax.axis_size("space")
    count = sum(block.shape[0] for block in blocks)
    picked = call(
        pick_kernel, jax.ShapeDtypeStruct((count, 2 * EDGE, blocks[0].shape[2]), F32), operands=len(blocks)
    )(*blocks)
    if size == 1:
        return picked
    if size == 2:
        return lax.ppermute(picked, "space", [(0, 1), (1, 0)])
    after = lax.ppermute(picked[:, :EDGE], "space", [(i, (i - 1) % size) for i in range(size)])
    before = lax.ppermute(picked[:, EDGE:], "space", [(i, (i + 1) % size) for i in range(size)])
    return jnp.concatenate([after, before], axis=1)


def pack_kernel(x_ref, keep_ref, send_ref):
    _, lo = pair_position()
    columns = x_ref.shape[2]
    half = columns // PAIR
    lane = lax.broadcasted_iota(jnp.int32, (x_ref.shape[1], LANES), 1)

    local = x_ref.shape[0]

    def body(q, carry):
        k = jnp.where(lo == 0, q, local - 1 - q)
        for ref, part in ((keep_ref, lo), (send_ref, 1 - lo)):
            begin = pl.multiple_of(part * half, LANES)
            right = pl.multiple_of((1 - part) * half, LANES)
            left = pl.multiple_of((1 - part) * half + half - LANES, LANES)
            ref[q, :, 0:half] = x_ref[k, :, pl.ds(begin, half)]
            ref[q, :, half:] = jnp.where(
                lane < LANES // 2, x_ref[k, :, pl.ds(right, LANES)], x_ref[k, :, pl.ds(left, LANES)]
            )
        return carry

    lax.fori_loop(0, local, body, 0)


def sum_of_neighbours(load, tiles, rows, use):
    lane = lax.broadcasted_iota(jnp.int32, (rows, LANES), 1)
    is_first, is_last = lane == 0, lane == LANES - 1
    center = load(0)
    from_left = pltpu.roll(load(tiles - 1), 1, 1)
    to_left = pltpu.roll(center, LANES - 1, 1)
    for t in range(tiles):
        following = load((t + 1) % tiles)
        shifted = pltpu.roll(center, 1, 1)
        next_to_left = pltpu.roll(following, LANES - 1, 1)
        west = jnp.where(is_first, from_left, shifted)
        east = jnp.where(is_last, next_to_left, to_left)
        north = pltpu.roll(center, 1, 0)
        south = pltpu.roll(center, rows - 1, 0)
        use(t, center, (north + south) + (west + east))
        center, from_left, to_left = following, shifted, next_to_left


def tile_of(t):
    return slice(t * LANES, (t + 1) * LANES)


def neighbours_of(k, first, count):
    gid = k + first
    is_first, is_last = gid == 0, gid == count - 1
    before = jnp.where(is_first, k, k - 1)
    after = jnp.where(is_last, k, k + 1)
    stretch = jnp.where(is_first | is_last, F32(count - 1), F32((count - 1) / 2.0))
    return before, after, stretch


def fold(value):
    return jnp.sum(value.reshape(-1, SUBLANES, LANES), axis=0)


def drift_pass(phi, drift, norms, low, high, first, count, own_rows, shift=0):
    rows = phi.shape[1]
    tiles = phi.shape[2] // LANES

    def body(k, carry):
        before, after, stretch = neighbours_of(k, first, count)
        sums = [jnp.zeros((SUBLANES, LANES), F32), jnp.zeros((SUBLANES, LANES), F32)]

        def use(t, center, total):
            force = total - center * (3.0 + center * center)
            drift[k, :, tile_of(t)] = force
            if t < tiles - 1 and norms is not None:
                step = phi[after, 0:own_rows, tile_of(t)] - phi[before, 0:own_rows, tile_of(t)]
                own = force[0:own_rows]
                sums[0] = sums[0] + fold(own * own)
                sums[1] = sums[1] + fold(step * step)

        sum_of_neighbours(lambda t: phi[k, :, tile_of(t)], tiles, rows, use)
        if norms is not None:
            norms[0, pl.ds(k - shift, 1), :] = jnp.sum(sums[0], axis=0, keepdims=True)
            norms[1, pl.ds(k - shift, 1), :] = jnp.sum(sums[1], axis=0, keepdims=True) * (stretch * stretch)
        return carry

    lax.fori_loop(low, high, body, 0)


def speeds_of(norms, speeds):
    force = jnp.sum(norms[0], axis=1, keepdims=True)
    path = jnp.sum(norms[1], axis=1, keepdims=True)
    value = jnp.sqrt(force + EPSILON) / jnp.sqrt(path + EPSILON)
    speeds[...] = jnp.broadcast_to(value, speeds.shape)


def theta_pass(phi, drift, speeds, theta, low, high, first, count):
    tiles = phi.shape[2] // LANES

    def body(k, carry):
        before, after, stretch = neighbours_of(k, first, count)
        scale = speeds[pl.ds(k, 1), :] * stretch
        for t in range(tiles):
            cols = tile_of(t)
            theta[k, :, cols] = scale * (phi[after, :, cols] - phi[before, :, cols]) - drift[k, :, cols]
        return carry

    lax.fori_loop(low, high, body, 0)


def update_pass(phi, speeds, theta, low, high, first, count, store):
    rows = phi.shape[1]
    tiles = phi.shape[2] // LANES

    def body(k, carry):
        before, after, stretch = neighbours_of(k, first, count)
        scale = speeds[pl.ds(k, 1), :] * stretch
        gid = k + first
        inside = (gid > 0) & (gid < count - 1)

        def use(t, center, total):
            cols = tile_of(t)
            value = phi[k, :, cols]
            descent = (
                scale * (theta[after, :, cols] - theta[before, :, cols])
                + total
                - (3.0 * center) * (1.0 + value * value)
            )
            store(k, t, jnp.where(inside, value + TIME_STEP * descent, value))

        sum_of_neighbours(lambda t: theta[k, :, tile_of(t)], tiles, rows, use)
        return carry

    lax.fori_loop(low, high, body, 0)


def chunk_of(q):
    return max(c for c in range(len(CHUNKS)) if CHUNKS[c] <= q)


def place(phi, at, image, edge_rows):
    rows = image.shape[0]
    phi[at, 0:rows, :] = image
    phi[at, rows:, :] = edge_rows


def inner_kernel(*refs, count):
    refs = list(refs)
    pick = lambda n: [refs.pop(0) for _ in range(n)]
    (keep,), recv = pick(1), pick(len(CHUNKS))
    near_early, near_late, edge_rows, phi, drift, norms = pick(6)
    local, rows, _ = keep.shape
    hi, lo = pair_position()
    first = hi * (PAIR * local) - LOW
    top = LOW + PAIR * local

    def own_at(part, q):
        return LOW + part * local + jnp.where(part == 0, q, local - 1 - q)

    for q in range(local):
        place(phi, own_at(lo, q), keep[q], edge_rows[q])
        place(phi, own_at(1 - lo, q), recv[chunk_of(q)][q - CHUNKS[chunk_of(q)]], edge_rows[local + q])
    phi[jnp.where(lo == 1, LOW - 1, top), 0:rows, :] = near_early[0]
    phi[jnp.where(lo == 1, top, LOW - 1), 0:rows, :] = near_late[0]
    drift_pass(phi, drift, norms, LOW, top, first, count, rows, LOW)


def outer_kernel(*refs, count):
    refs = list(refs)
    pick = lambda n: [refs.pop(0) for _ in range(n)]
    _, _, near_early, far_early = pick(4)
    near_late, far_late = pick(len(CHUNKS)), pick(len([c for c in range(len(CHUNKS)) if far_count(c)]))
    rows_early, rows_late, phi, drift = pick(4)
    local, rows, _ = near_early.shape
    hi, lo = pair_position()
    first = hi * (PAIR * local) - LOW
    top = LOW + PAIR * local
    skipped = len(CHUNKS) - len(far_late)
    for q in range(local):
        low_at, high_at = LOW - 1 - q, top + q
        place(phi, jnp.where(lo == 1, low_at, high_at), near_early[q], rows_early[PAIR * local + q])
        late = near_late[chunk_of(q)][q - CHUNKS[chunk_of(q)]]
        place(phi, jnp.where(lo == 1, high_at, low_at), late, rows_late[q])
    for i in range(FAR):
        low_at, high_at = LOW - 1 - local - i, top + local + i
        q = local - 1 - i
        late = far_late[chunk_of(q) - skipped].at[q - max(CHUNKS[chunk_of(q)], local - FAR)]
        late_rows = rows_late.at[local + FAR - 1 - i]
        early, early_rows = far_early.at[FAR - 1 - i], rows_early.at[(PAIR + 1) * local + FAR - 1 - i]

        @pl.when(lo == 1)
        def _():
            if high_at < phi.shape[0]:
                place(phi, high_at, early[...], early_rows[...])
            if low_at >= 0:
                place(phi, low_at, late[...], late_rows[...])

        @pl.when(lo == 0)
        def _():
            if high_at < phi.shape[0]:
                place(phi, high_at, late[...], late_rows[...])
            if low_at >= 0:
                place(phi, low_at, early[...], early_rows[...])

    drift_pass(phi, drift, None, 1, LOW, first, count, rows)
    drift_pass(phi, drift, None, top, phi.shape[0] - 1, first, count, rows)


def far_count(chunk):
    ends = CHUNKS[1:] + (CHUNKS[-1] + FAR,)
    return max(0, ends[chunk] - max(CHUNKS[chunk], 2 * ITERS - FAR))


def middle_kernel(phi, drift, norms, new_phi, new_drift, new_norms, theta, speeds, *, count, local, rows, done):
    hi, _ = pair_position()
    first = hi * (PAIR * local) - LOW
    window = phi.shape[0]
    speeds_of(norms, speeds)
    theta_pass(phi, drift, speeds, theta, done + 1, window - done - 1, first, count)

    def store(k, t, value):
        new_phi[k, :, tile_of(t)] = value

    update_pass(phi, speeds, theta, done + 2, window - done - 2, first, count, store)
    new_norms[...] = jnp.zeros(new_norms.shape, F32)
    drift_pass(new_phi, new_drift, new_norms, done + 3, window - done - 3, first, count, rows)


def last_kernel(phi, drift, norms, final, squares, theta, speeds, *, count, local, rows, done):
    hi, _ = pair_position()
    first = hi * (PAIR * local) - LOW
    window = phi.shape[0]
    tiles = final.shape[2] // LANES
    shift = LOW - REACH
    speeds_of(norms, speeds)
    theta_pass(phi, drift, speeds, theta, done + 1, window - done - 1, first, count)

    def store(k, t, value):
        if t < tiles:
            final[k - shift, :, tile_of(t)] = value[0:rows]

    update_pass(phi, speeds, theta, shift, shift + final.shape[0], first, count, store)
    position = (
        lax.broadcasted_iota(jnp.int32, squares.shape, 0) * LANES
        + lax.broadcasted_iota(jnp.int32, squares.shape, 1)
    )

    def body(i, total):
        k = REACH + i
        acc = jnp.zeros((SUBLANES, LANES), F32)
        for t in range(tiles):
            diff = final[k, :, tile_of(t)] - final[k - 1, :, tile_of(t)]
            acc = acc + fold(diff * diff)
        amount = jnp.sum(jnp.sum(acc, axis=0, keepdims=True), axis=1, keepdims=True)
        return total + jnp.where(position == LOW + i + first, amount, 0.0)

    squares[...] = lax.fori_loop(0, PAIR * local, body, jnp.zeros(squares.shape, F32))


def combine_kernel(bracket, window, squares, out, *scratch, count, own):
    hi, lo = pair_position()
    part = lo if own else 1 - lo
    whole, out = out, scratch[0] if own else out
    local, _, half = out.shape
    tiles = half // LANES
    begin = hi * (PAIR * local)
    position = (
        lax.broadcasted_iota(jnp.int32, squares.shape, 0) * LANES
        + lax.broadcasted_iota(jnp.int32, squares.shape, 1)
    )
    counted = (position >= 1) & (position < count)
    segments = jnp.where(counted, jnp.sqrt(squares[...] + EPSILON), 0.0)

    def total(value):
        return jnp.sum(jnp.sum(value, axis=0, keepdims=True), axis=1, keepdims=True)

    length = total(segments)
    weights = []
    for i in range(local):
        b = bracket[i]
        j = begin + part * local + i
        arc = total(jnp.where(position <= b, segments, 0.0))
        segment = total(jnp.where(position == b + 1, segments, 0.0))
        target = length * lax.convert_element_type(j, F32) / F32(count - 1)
        weights.append((target - arc) / segment)
    for i in range(local):
        at = bracket[i] - begin + REACH
        for t in range(tiles):
            base = window[at, :, tile_of(t)]
            out[i, :, tile_of(t)] = base + weights[i] * (window[at + 1, :, tile_of(t)] - base)
    if own:
        copy_half(out, whole, lo, scratch[1])


def copy_half(half_ref, whole, part, sem):
    half = half_ref.shape[2]
    copy = pltpu.make_async_copy(half_ref, whole.at[:, :, pl.ds(pl.multiple_of(part * half, LANES), half)], sem)
    copy.start()
    copy.wait()


def finish_kernel(whole_in, other, whole, sem):
    _, lo = pair_position()
    copy_half(other, whole, 1 - lo, sem)


def per_device(path, bracket):
    local, rows, columns = path.shape
    devices = lax.axis_size("img")
    count = local * devices
    half = columns // PAIR
    wide = half + LANES
    window = LOW + PAIR * local + HIGH
    if devices & (devices - 1) or local != 2 * ITERS or count > SUBLANES * LANES or rows % SUBLANES:
        raise ValueError("unsupported sizes")
    shape = functools.partial(jax.ShapeDtypeStruct, dtype=F32)
    block = shape((local, rows, wide))
    ahead = [(i, i + PAIR) for i in range(devices - PAIR)]
    back = [(target, source) for source, target in ahead]
    move = lambda value, up, down: lax.ppermute(
        value, "img",
        [p for p in ahead if p[0] % PAIR in up] + [p for p in back if p[0] % PAIR in down],
    )
    keep, send = call(pack_kernel, (block, block), operands=1)(path)
    ends = CHUNKS[1:] + (local,)
    recv = [swap_pairs(send[a:b]) for a, b in zip(CHUNKS, ends)]
    other_bracket = swap_pairs(bracket)
    near_early = move(keep, (1,), (0,))
    far_early = move(keep[local - FAR :], (0,), (1,))
    near_late = [move(value, (0,), (1,)) for value in recv]
    far_late = [
        move(value[max(0, local - FAR - a) :], (1,), (0,))
        for i, (a, value) in enumerate(zip(CHUNKS, recv)) if far_count(i)
    ]
    rows_early = neighbour_rows([keep] + recv + [near_early, far_early])
    rows_late = neighbour_rows(near_late + far_late)
    held = shape((window, rows + 2 * EDGE, wide))
    lines = -(-window // SUBLANES) * SUBLANES
    norm_shape = shape((2, lines, LANES))
    operands = [keep] + recv + [near_early, near_late[0], rows_early]
    phi, drift, norms = call(
        functools.partial(inner_kernel, count=count), (held, held, shape((2, PAIR * local, LANES))),
        operands=len(operands),
    )(*operands)
    norms = small_sum(norms, (1,))
    low_norms = lax.ppermute(norms, "img", ahead)
    high_norms = lax.ppermute(norms, "img", back)
    operands = [phi, drift, near_early, far_early] + near_late + far_late + [rows_early, rows_late]
    phi, drift = call(
        functools.partial(outer_kernel, count=count), (held, held), operands=len(operands), aliases={0: 0, 1: 1}
    )(*operands)
    pad = jnp.zeros((2, lines - window, LANES), F32)
    norms = jnp.concatenate([low_norms[:, PAIR * local - LOW :], norms, high_norms[:, :HIGH], pad], axis=1)
    scratch = [pltpu.VMEM(held.shape, F32), pltpu.VMEM((lines, LANES), F32)]
    for iteration in range(ITERS - 1):
        if iteration:
            norms = small_sum(norms, (1,))
        phi, drift, norms = call(
            functools.partial(middle_kernel, count=count, local=local, rows=rows, done=2 * iteration),
            (held, held, norm_shape), scratch=scratch, operands=3,
        )(phi, drift, norms)
    norms = small_sum(norms, (1,))
    final, squares = call(
        functools.partial(last_kernel, count=count, local=local, rows=rows, done=2 * (ITERS - 1)),
        (shape((PAIR * local + 2 * REACH + 1, rows, half)), shape((SUBLANES, LANES))),
        scratch=scratch, operands=3,
    )(phi, drift, norms)
    steps = []
    step = 1
    while step < devices:
        steps.append(step)
        step *= 2
    squares = small_sum(squares, steps)
    half_block = (local, rows, half)
    whole = shape((local, rows, columns))
    in_smem, in_vmem, in_hbm = (pl.BlockSpec(memory_space=m) for m in (pltpu.SMEM, pltpu.VMEM, pl.ANY))
    other = swap_pairs(
        call(functools.partial(combine_kernel, count=count, own=False), shape(half_block), smem=1, operands=2)(
            other_bracket, final, squares
        )
    )
    mine = pl.pallas_call(
        functools.partial(combine_kernel, count=count, own=True),
        out_shape=whole,
        in_specs=[in_smem, in_vmem, in_vmem],
        out_specs=in_hbm,
        scratch_shapes=[pltpu.VMEM(half_block, F32), pltpu.SemaphoreType.DMA],
        compiler_params=pltpu.CompilerParams(vmem_limit_bytes=VMEM_LIMIT),
    )(bracket, final, squares)
    return pl.pallas_call(
        finish_kernel,
        out_shape=whole,
        in_specs=[in_hbm, in_vmem],
        out_specs=in_hbm,
        scratch_shapes=[pltpu.SemaphoreType.DMA],
        input_output_aliases={0: 0},
        compiler_params=pltpu.CompilerParams(vmem_limit_bytes=VMEM_LIMIT),
    )(mine, other)


def solution(mesh):
    return jax.shard_map(
        per_device,
        mesh=mesh,
        in_specs=(P(("groups", "img"), "space", None), P(("groups", "img"))),
        out_specs=P(("groups", "img"), "space", None),
        check_vma=False,
    )
```

```python
import functools

import jax
import jax.numpy as jnp
from jax import lax
from jax.experimental import pallas as pl
from jax.experimental.pallas import tpu as pltpu
from jax.sharding import PartitionSpec as P


REACH = 2
ITERS = 2
TIME_STEP = 0.002
EPSILON = 1e-06

LANES = 128
SUBLANES = 8
PAIR = 2
LOW = 2 * ITERS + REACH
HIGH = 2 * ITERS + REACH + 1
FAR = 3
EDGE = 2 * ITERS
CHUNKS = (0, 2)
VMEM_LIMIT = 4 * 1024 * 1024

F32 = jnp.float32


def call(kernel, out_shapes, scratch=(), smem=0, operands=0, aliases=None):
    specs = [pl.BlockSpec(memory_space=pltpu.SMEM)] * smem
    specs += [pl.BlockSpec(memory_space=pltpu.VMEM)] * operands
    return pl.pallas_call(
        kernel,
        out_shape=out_shapes,
        in_specs=specs,
        out_specs=jax.tree.map(lambda _: pl.BlockSpec(memory_space=pltpu.VMEM), out_shapes),
        scratch_shapes=list(scratch),
        input_output_aliases=aliases or {},
        compiler_params=pltpu.CompilerParams(vmem_limit_bytes=VMEM_LIMIT),
    )


def pair_position():
    index = lax.axis_index("img")
    return lax.div(index, PAIR), lax.rem(index, PAIR)


def swap_pairs(value):
    count = lax.axis_size("img")
    return lax.ppermute(value, "img", [(i, i ^ 1) for i in range(count)])


def small_sum(value, steps):
    size = lax.axis_size("space")
    if size & (size - 1) == 0:
        step = 1
        while step < size:
            value = value + lax.ppermute(value, "space", [(i, i ^ step) for i in range(size)])
            step *= 2
    else:
        value = lax.psum(value, "space")
    count = lax.axis_size("img")
    for step in steps:
        value = value + lax.ppermute(value, "img", [(i, i ^ step) for i in range(count)])
    return value


def pick_kernel(*refs):
    *blocks, picked = refs
    at = 0
    for block in blocks:
        for i in range(block.shape[0]):
            picked[at, 0:EDGE, :] = block[i, 0:EDGE, :]
            picked[at, EDGE:, :] = block[i, block.shape[1] - EDGE :, :]
            at += 1


def neighbour_rows(blocks):
    size = lax.axis_size("space")
    count = sum(block.shape[0] for block in blocks)
    picked = call(
        pick_kernel, jax.ShapeDtypeStruct((count, 2 * EDGE, blocks[0].shape[2]), F32), operands=len(blocks)
    )(*blocks)
    if size == 1:
        return picked
    if size == 2:
        return lax.ppermute(picked, "space", [(0, 1), (1, 0)])
    after = lax.ppermute(picked[:, :EDGE], "space", [(i, (i - 1) % size) for i in range(size)])
    before = lax.ppermute(picked[:, EDGE:], "space", [(i, (i + 1) % size) for i in range(size)])
    return jnp.concatenate([after, before], axis=1)


def pack_kernel(x_ref, keep_ref, send_ref):
    _, lo = pair_position()
    columns = x_ref.shape[2]
    half = columns // PAIR
    lane = lax.broadcasted_iota(jnp.int32, (x_ref.shape[1], LANES), 1)

    local = x_ref.shape[0]

    def body(q, carry):
        k = jnp.where(lo == 0, q, local - 1 - q)
        for ref, part in ((keep_ref, lo), (send_ref, 1 - lo)):
            begin = pl.multiple_of(part * half, LANES)
            right = pl.multiple_of((1 - part) * half, LANES)
            left = pl.multiple_of((1 - part) * half + half - LANES, LANES)
            ref[q, :, 0:half] = x_ref[k, :, pl.ds(begin, half)]
            ref[q, :, half:] = jnp.where(
                lane < LANES // 2, x_ref[k, :, pl.ds(right, LANES)], x_ref[k, :, pl.ds(left, LANES)]
            )
        return carry

    lax.fori_loop(0, local, body, 0)


def sum_of_neighbours(load, tiles, rows, use):
    lane = lax.broadcasted_iota(jnp.int32, (rows, LANES), 1)
    is_first, is_last = lane == 0, lane == LANES - 1
    center = load(0)
    from_left = pltpu.roll(load(tiles - 1), 1, 1)
    to_left = pltpu.roll(center, LANES - 1, 1)
    for t in range(tiles):
        following = load((t + 1) % tiles)
        shifted = pltpu.roll(center, 1, 1)
        next_to_left = pltpu.roll(following, LANES - 1, 1)
        west = jnp.where(is_first, from_left, shifted)
        east = jnp.where(is_last, next_to_left, to_left)
        north = pltpu.roll(center, 1, 0)
        south = pltpu.roll(center, rows - 1, 0)
        use(t, center, (north + south) + (west + east))
        center, from_left, to_left = following, shifted, next_to_left


def tile_of(t):
    return slice(t * LANES, (t + 1) * LANES)


def neighbours_of(k, first, count):
    gid = k + first
    is_first, is_last = gid == 0, gid == count - 1
    before = jnp.where(is_first, k, k - 1)
    after = jnp.where(is_last, k, k + 1)
    stretch = jnp.where(is_first | is_last, F32(count - 1), F32((count - 1) / 2.0))
    return before, after, stretch


def fold(value):
    return jnp.sum(value.reshape(-1, SUBLANES, LANES), axis=0)


def drift_pass(phi, drift, norms, low, high, first, count, own_rows, shift=0):
    rows = phi.shape[1]
    tiles = phi.shape[2] // LANES

    def body(k, carry):
        before, after, stretch = neighbours_of(k, first, count)
        sums = [jnp.zeros((SUBLANES, LANES), F32), jnp.zeros((SUBLANES, LANES), F32)]

        def use(t, center, total):
            force = total - center * (3.0 + center * center)
            drift[k, :, tile_of(t)] = force
            if t < tiles - 1 and norms is not None:
                step = phi[after, 0:own_rows, tile_of(t)] - phi[before, 0:own_rows, tile_of(t)]
                own = force[0:own_rows]
                sums[0] = sums[0] + fold(own * own)
                sums[1] = sums[1] + fold(step * step)

        sum_of_neighbours(lambda t: phi[k, :, tile_of(t)], tiles, rows, use)
        if norms is not None:
            norms[0, pl.ds(k - shift, 1), :] = jnp.sum(sums[0], axis=0, keepdims=True)
            norms[1, pl.ds(k - shift, 1), :] = jnp.sum(sums[1], axis=0, keepdims=True) * (stretch * stretch)
        return carry

    lax.fori_loop(low, high, body, 0)


def speeds_of(norms, speeds):
    force = jnp.sum(norms[0], axis=1, keepdims=True)
    path = jnp.sum(norms[1], axis=1, keepdims=True)
    value = jnp.sqrt(force + EPSILON) / jnp.sqrt(path + EPSILON)
    speeds[...] = jnp.broadcast_to(value, speeds.shape)


def theta_pass(phi, speeds, theta, low, high, first, count, shift=0):
    tiles = phi.shape[2] // LANES

    def body(k, carry):
        before, after, stretch = neighbours_of(k, first, count)
        scale = speeds[pl.ds(k - shift, 1), :] * stretch
        for t in range(tiles):
            cols = tile_of(t)
            theta[k, :, cols] = scale * (phi[after, :, cols] - phi[before, :, cols]) - theta[k, :, cols]
        return carry

    lax.fori_loop(low, high, body, 0)


def update_pass(phi, speeds, theta, low, high, first, count, store, shift=0):
    rows = phi.shape[1]
    tiles = phi.shape[2] // LANES

    def body(k, carry):
        before, after, stretch = neighbours_of(k, first, count)
        scale = speeds[pl.ds(k - shift, 1), :] * stretch
        gid = k + first
        inside = (gid > 0) & (gid < count - 1)

        def use(t, center, total):
            cols = tile_of(t)
            value = phi[k, :, cols]
            descent = (
                scale * (theta[after, :, cols] - theta[before, :, cols])
                + total
                - (3.0 * center) * (1.0 + value * value)
            )
            store(k, t, jnp.where(inside, value + TIME_STEP * descent, value))

        sum_of_neighbours(lambda t: theta[k, :, tile_of(t)], tiles, rows, use)
        return carry

    lax.fori_loop(low, high, body, 0)


def chunk_of(q):
    return max(c for c in range(len(CHUNKS)) if CHUNKS[c] <= q)


def place(phi, at, image, edge_rows):
    rows = image.shape[0]
    phi[at, 0:rows, :] = image
    phi[at, rows:, :] = edge_rows


def inner_kernel(*refs, count):
    refs = list(refs)
    pick = lambda n: [refs.pop(0) for _ in range(n)]
    (keep,), recv = pick(1), pick(len(CHUNKS))
    near_early, near_late, edge_rows, phi, drift, norms = pick(6)
    local, rows, _ = keep.shape
    hi, lo = pair_position()
    first = hi * (PAIR * local) - LOW
    top = LOW + PAIR * local

    def own_at(part, q):
        return LOW + part * local + jnp.where(part == 0, q, local - 1 - q)

    for q in range(local):
        place(phi, own_at(lo, q), keep[q], edge_rows[q])
        place(phi, own_at(1 - lo, q), recv[chunk_of(q)][q - CHUNKS[chunk_of(q)]], edge_rows[local + q])
        low_at, high_at = LOW - 1 - q, top + q
        place(phi, jnp.where(lo == 1, low_at, high_at), near_early[q], edge_rows[2 * local + q])
        if q < near_late.shape[0]:
            place(phi, jnp.where(lo == 1, high_at, low_at), near_late[q], edge_rows[3 * local + q])
    drift_pass(phi, drift, norms, LOW - 1, top + 1, first, count, rows, LOW - 1)


def middle_inner_kernel(_, __, norms, phi, theta, new_phi, new_drift, new_norms, speeds, *, count, local, rows):
    hi, _ = pair_position()
    first = hi * (PAIR * local) - LOW
    top = LOW + PAIR * local
    speeds_of(norms, speeds)
    theta_pass(phi, speeds, theta, LOW - 1, top + 1, first, count, LOW - 1)

    def store(k, t, value):
        new_phi[k, :, tile_of(t)] = value

    update_pass(phi, speeds, theta, LOW, top, first, count, store, LOW - 1)
    new_norms[...] = jnp.zeros(new_norms.shape, F32)
    drift_pass(new_phi, new_drift, new_norms, LOW + 1, top - 1, first, count, rows)


def middle_outer_kernel(norms, near_late, far_early, far_late, rows_early, rows_late, *refs, count, local):
    phi, theta, new_phi, new_drift, new_norms, speeds = refs[5:]
    rows = near_late.shape[1]
    hi, lo = pair_position()
    first = hi * (PAIR * local) - LOW
    top = LOW + PAIR * local
    window = phi.shape[0]
    done = CHUNKS[-1]
    for q in range(done, local):
        place(phi, jnp.where(lo == 1, top + q, LOW - 1 - q), near_late[q - done], rows_late[q - done])
    for i in range(FAR):
        low_at, high_at = LOW - 1 - local - i, top + local + i
        at = FAR - 1 - i
        late, late_rows = far_late.at[at], rows_late.at[local - done + at]
        early, early_rows = far_early.at[at], rows_early.at[3 * local + done + at]

        @pl.when(lo == 1)
        def _():
            if high_at < window:
                place(phi, high_at, early[...], early_rows[...])
            if low_at >= 0:
                place(phi, low_at, late[...], late_rows[...])

        @pl.when(lo == 0)
        def _():
            if high_at < window:
                place(phi, high_at, late[...], late_rows[...])
            if low_at >= 0:
                place(phi, low_at, early[...], early_rows[...])

    def store(k, t, value):
        new_phi[k, :, tile_of(t)] = value

    speeds_of(norms, speeds)
    for low, high in ((1, LOW - 1), (top + 1, window - 1)):
        drift_pass(phi, theta, None, low, high, first, count, rows)
        theta_pass(phi, speeds, theta, low, high, first, count)
    for low, high in ((2, LOW), (top, window - 2)):
        update_pass(phi, speeds, theta, low, high, first, count, store)
    for low, high in ((3, LOW + 1), (top - 1, window - 3)):
        drift_pass(new_phi, new_drift, new_norms, low, high, first, count, rows)


def last_kernel(phi, _, norms, final, squares, theta, speeds, *, count, local, rows, done):
    hi, _ = pair_position()
    first = hi * (PAIR * local) - LOW
    window = phi.shape[0]
    tiles = final.shape[2] // LANES
    shift = LOW - REACH
    speeds_of(norms, speeds)
    theta_pass(phi, speeds, theta, done + 1, window - done - 1, first, count)

    def store(k, t, value):
        if t < tiles:
            final[k - shift, :, tile_of(t)] = value[0:rows]

    update_pass(phi, speeds, theta, shift, shift + final.shape[0], first, count, store)
    position = (
        lax.broadcasted_iota(jnp.int32, squares.shape, 0) * LANES
        + lax.broadcasted_iota(jnp.int32, squares.shape, 1)
    )

    def body(i, total):
        k = REACH + i
        acc = jnp.zeros((SUBLANES, LANES), F32)
        for t in range(tiles):
            diff = final[k, :, tile_of(t)] - final[k - 1, :, tile_of(t)]
            acc = acc + fold(diff * diff)
        amount = jnp.sum(jnp.sum(acc, axis=0, keepdims=True), axis=1, keepdims=True)
        return total + jnp.where(position == LOW + i + first, amount, 0.0)

    squares[...] = lax.fori_loop(0, PAIR * local, body, jnp.zeros(squares.shape, F32))


def combine_kernel(bracket, window, squares, out, *scratch, count, own):
    hi, lo = pair_position()
    part = lo if own else 1 - lo
    whole, out = out, scratch[0] if own else out
    local, _, half = out.shape
    tiles = half // LANES
    begin = hi * (PAIR * local)
    position = (
        lax.broadcasted_iota(jnp.int32, squares.shape, 0) * LANES
        + lax.broadcasted_iota(jnp.int32, squares.shape, 1)
    )
    counted = (position >= 1) & (position < count)
    segments = jnp.where(counted, jnp.sqrt(squares[...] + EPSILON), 0.0)

    def total(value):
        return jnp.sum(jnp.sum(value, axis=0, keepdims=True), axis=1, keepdims=True)

    length = total(segments)
    weights = []
    for i in range(local):
        b = bracket[i]
        j = begin + part * local + i
        arc = total(jnp.where(position <= b, segments, 0.0))
        segment = total(jnp.where(position == b + 1, segments, 0.0))
        target = length * lax.convert_element_type(j, F32) / F32(count - 1)
        weights.append((target - arc) / segment)
    for i in range(local):
        at = bracket[i] - begin + REACH
        for t in range(tiles):
            base = window[at, :, tile_of(t)]
            out[i, :, tile_of(t)] = base + weights[i] * (window[at + 1, :, tile_of(t)] - base)
    if own:
        copy_half(out, whole, lo, scratch[1])


def copy_half(half_ref, whole, part, sem):
    half = half_ref.shape[2]
    copy = pltpu.make_async_copy(half_ref, whole.at[:, :, pl.ds(pl.multiple_of(part * half, LANES), half)], sem)
    copy.start()
    copy.wait()


def finish_kernel(whole_in, other, whole, sem):
    _, lo = pair_position()
    copy_half(other, whole, 1 - lo, sem)


def per_device(path, bracket):
    local, rows, columns = path.shape
    devices = lax.axis_size("img")
    count = local * devices
    half = columns // PAIR
    wide = half + LANES
    window = LOW + PAIR * local + HIGH
    if devices & (devices - 1) or ITERS != 2 or local != 2 * ITERS or count > SUBLANES * LANES or rows % SUBLANES:
        raise ValueError("unsupported sizes")
    shape = functools.partial(jax.ShapeDtypeStruct, dtype=F32)
    block = shape((local, rows, wide))
    ahead = [(i, i + PAIR) for i in range(devices - PAIR)]
    back = [(target, source) for source, target in ahead]
    move = lambda value, up, down: lax.ppermute(
        value, "img",
        [p for p in ahead if p[0] % PAIR in up] + [p for p in back if p[0] % PAIR in down],
    )
    keep, send = call(pack_kernel, (block, block), operands=1)(path)
    ends = CHUNKS[1:] + (local,)
    recv = [swap_pairs(send[a:b]) for a, b in zip(CHUNKS, ends)]
    other_bracket = swap_pairs(bracket)
    near_early = move(keep, (1,), (0,))
    far_early = move(keep[local - FAR :], (0,), (1,))
    near_late = [move(value, (0,), (1,)) for value in recv]
    far_late = move(jnp.concatenate(recv, axis=0)[local - FAR :], (1,), (0,))
    rows_early = neighbour_rows([keep] + recv + [near_early, near_late[0], far_early])
    rows_late = neighbour_rows([near_late[1], far_late])
    held = shape((window, rows + 2 * EDGE, wide))
    lines = -(-window // SUBLANES) * SUBLANES
    norm_shape = shape((2, lines, LANES))
    operands = [keep] + recv + [near_early, near_late[0], rows_early]
    inside = PAIR * local + 2
    inside_lines = -(-inside // SUBLANES) * SUBLANES
    phi, drift, norms = call(
        functools.partial(inner_kernel, count=count), (held, held, shape((2, inside_lines, LANES))),
        operands=len(operands),
    )(*operands)
    norms = small_sum(norms, (1,))
    own_norms = norms[:, 1 : inside - 1]
    low_norms = lax.ppermute(own_norms, "img", ahead)
    high_norms = lax.ppermute(own_norms, "img", back)
    state = call(
        functools.partial(middle_inner_kernel, count=count, local=local, rows=rows),
        (held, held, held, held, norm_shape), scratch=[pltpu.VMEM((inside_lines, LANES), F32)],
        operands=3, aliases={0: 0, 1: 1},
    )(phi, drift, norms)
    pad = jnp.zeros((2, lines - window, LANES), F32)
    norms = jnp.concatenate([low_norms[:, PAIR * local - LOW :], own_norms, high_norms[:, :HIGH], pad], axis=1)
    operands = [norms, near_late[1], far_early, far_late, rows_early, rows_late]
    _, _, phi, drift, norms = call(
        functools.partial(middle_outer_kernel, count=count, local=local),
        (held, held, held, held, norm_shape), scratch=[pltpu.VMEM((lines, LANES), F32)],
        operands=len(operands) + len(state), aliases={len(operands) + i: i for i in range(len(state))},
    )(*operands, *state)
    scratch = [pltpu.VMEM((lines, LANES), F32)]
    norms = small_sum(norms, (1,))
    final, squares, _ = call(
        functools.partial(last_kernel, count=count, local=local, rows=rows, done=2 * (ITERS - 1)),
        (shape((PAIR * local + 2 * REACH + 1, rows, half)), shape((SUBLANES, LANES)), held),
        scratch=scratch, operands=3, aliases={1: 2},
    )(phi, drift, norms)
    steps = []
    step = 1
    while step < devices:
        steps.append(step)
        step *= 2
    squares = small_sum(squares, steps)
    half_block = (local, rows, half)
    whole = shape((local, rows, columns))
    in_smem, in_vmem, in_hbm = (pl.BlockSpec(memory_space=m) for m in (pltpu.SMEM, pltpu.VMEM, pl.ANY))
    other = swap_pairs(
        call(functools.partial(combine_kernel, count=count, own=False), shape(half_block), smem=1, operands=2)(
            other_bracket, final, squares
        )
    )
    mine = pl.pallas_call(
        functools.partial(combine_kernel, count=count, own=True),
        out_shape=whole,
        in_specs=[in_smem, in_vmem, in_vmem],
        out_specs=in_hbm,
        scratch_shapes=[pltpu.VMEM(half_block, F32), pltpu.SemaphoreType.DMA],
        compiler_params=pltpu.CompilerParams(vmem_limit_bytes=VMEM_LIMIT),
    )(bracket, final, squares)
    return pl.pallas_call(
        finish_kernel,
        out_shape=whole,
        in_specs=[in_hbm, in_vmem],
        out_specs=in_hbm,
        scratch_shapes=[pltpu.SemaphoreType.DMA],
        input_output_aliases={0: 0},
        compiler_params=pltpu.CompilerParams(vmem_limit_bytes=VMEM_LIMIT),
    )(mine, other)


def solution(mesh):
    return jax.shard_map(
        per_device,
        mesh=mesh,
        in_specs=(P(("groups", "img"), "space", None), P(("groups", "img"))),
        out_specs=P(("groups", "img"), "space", None),
        check_vma=False,
    )
```

```python
import functools

import jax
import jax.numpy as jnp
from jax import lax
from jax.experimental import pallas as pl
from jax.experimental.pallas import tpu as pltpu
from jax.sharding import PartitionSpec as P


REACH = 2
ITERS = 2
TIME_STEP = 0.002
EPSILON = 1e-06

LANES = 128
SUBLANES = 8
PAIR = 2
LOW = 2 * ITERS + REACH
HIGH = 2 * ITERS + REACH + 1
FAR = 3
SHARED = 2
EDGE = 2 * ITERS
CHUNKS = (0, 2)
VMEM_LIMIT = 4 * 1024 * 1024

F32 = jnp.float32


def call(kernel, out_shapes, scratch=(), smem=0, operands=0, aliases=None):
    specs = [pl.BlockSpec(memory_space=pltpu.SMEM)] * smem
    specs += [pl.BlockSpec(memory_space=pltpu.VMEM)] * operands
    return pl.pallas_call(
        kernel,
        out_shape=out_shapes,
        in_specs=specs,
        out_specs=jax.tree.map(lambda _: pl.BlockSpec(memory_space=pltpu.VMEM), out_shapes),
        scratch_shapes=list(scratch),
        input_output_aliases=aliases or {},
        compiler_params=pltpu.CompilerParams(vmem_limit_bytes=VMEM_LIMIT),
    )


def pair_position():
    index = lax.axis_index("img")
    return lax.div(index, PAIR), lax.rem(index, PAIR)


def swap_pairs(value):
    count = lax.axis_size("img")
    return lax.ppermute(value, "img", [(i, i ^ 1) for i in range(count)])


def small_sum(value, steps):
    size = lax.axis_size("space")
    if size & (size - 1) == 0:
        step = 1
        while step < size:
            value = value + lax.ppermute(value, "space", [(i, i ^ step) for i in range(size)])
            step *= 2
    else:
        value = lax.psum(value, "space")
    count = lax.axis_size("img")
    for step in steps:
        value = value + lax.ppermute(value, "img", [(i, i ^ step) for i in range(count)])
    return value


def pick_kernel(*refs):
    *blocks, picked = refs
    at = 0
    for block in blocks:
        for i in range(block.shape[0]):
            picked[at, 0:EDGE, :] = block[i, 0:EDGE, :]
            picked[at, EDGE:, :] = block[i, block.shape[1] - EDGE :, :]
            at += 1


def neighbour_rows(blocks):
    size = lax.axis_size("space")
    count = sum(block.shape[0] for block in blocks)
    picked = call(
        pick_kernel, jax.ShapeDtypeStruct((count, 2 * EDGE, blocks[0].shape[2]), F32), operands=len(blocks)
    )(*blocks)
    if size == 1:
        return picked
    if size == 2:
        return lax.ppermute(picked, "space", [(0, 1), (1, 0)])
    after = lax.ppermute(picked[:, :EDGE], "space", [(i, (i - 1) % size) for i in range(size)])
    before = lax.ppermute(picked[:, EDGE:], "space", [(i, (i + 1) % size) for i in range(size)])
    return jnp.concatenate([after, before], axis=1)


def pack_kernel(x_ref, keep_ref, send_ref):
    _, lo = pair_position()
    columns = x_ref.shape[2]
    half = columns // PAIR
    lane = lax.broadcasted_iota(jnp.int32, (x_ref.shape[1], LANES), 1)

    local = x_ref.shape[0]

    def body(q, carry):
        k = jnp.where(lo == 0, q, local - 1 - q)
        for ref, part in ((keep_ref, lo), (send_ref, 1 - lo)):
            begin = pl.multiple_of(part * half, LANES)
            right = pl.multiple_of((1 - part) * half, LANES)
            left = pl.multiple_of((1 - part) * half + half - LANES, LANES)
            ref[q, :, 0:half] = x_ref[k, :, pl.ds(begin, half)]
            ref[q, :, half:] = jnp.where(
                lane < LANES // 2, x_ref[k, :, pl.ds(right, LANES)], x_ref[k, :, pl.ds(left, LANES)]
            )
        return carry

    lax.fori_loop(0, local, body, 0)


def sum_of_neighbours(load, tiles, rows, use):
    lane = lax.broadcasted_iota(jnp.int32, (rows, LANES), 1)
    is_first, is_last = lane == 0, lane == LANES - 1
    center = load(0)
    from_left = pltpu.roll(load(tiles - 1), 1, 1)
    to_left = pltpu.roll(center, LANES - 1, 1)
    for t in range(tiles):
        following = load((t + 1) % tiles)
        shifted = pltpu.roll(center, 1, 1)
        next_to_left = pltpu.roll(following, LANES - 1, 1)
        west = jnp.where(is_first, from_left, shifted)
        east = jnp.where(is_last, next_to_left, to_left)
        north = pltpu.roll(center, 1, 0)
        south = pltpu.roll(center, rows - 1, 0)
        use(t, center, (north + south) + (west + east))
        center, from_left, to_left = following, shifted, next_to_left


def tile_of(t):
    return slice(t * LANES, (t + 1) * LANES)


def neighbours_of(k, first, count):
    gid = k + first
    is_first, is_last = gid == 0, gid == count - 1
    before = jnp.where(is_first, k, k - 1)
    after = jnp.where(is_last, k, k + 1)
    stretch = jnp.where(is_first | is_last, F32(count - 1), F32((count - 1) / 2.0))
    return before, after, stretch


def fold(value):
    return jnp.sum(value.reshape(-1, SUBLANES, LANES), axis=0)


def drift_pass(phi, drift, norms, low, high, first, count, own_rows, shift=0):
    rows = phi.shape[1]
    tiles = phi.shape[2] // LANES

    def body(k, carry):
        before, after, stretch = neighbours_of(k, first, count)
        sums = [jnp.zeros((SUBLANES, LANES), F32), jnp.zeros((SUBLANES, LANES), F32)]

        def use(t, center, total):
            force = total - center * (3.0 + center * center)
            drift[k, :, tile_of(t)] = force
            if t < tiles - 1 and norms is not None:
                step = phi[after, 0:own_rows, tile_of(t)] - phi[before, 0:own_rows, tile_of(t)]
                own = force[0:own_rows]
                sums[0] = sums[0] + fold(own * own)
                sums[1] = sums[1] + fold(step * step)

        sum_of_neighbours(lambda t: phi[k, :, tile_of(t)], tiles, rows, use)
        if norms is not None:
            norms[0, pl.ds(k - shift, 1), :] = jnp.sum(sums[0], axis=0, keepdims=True)
            norms[1, pl.ds(k - shift, 1), :] = jnp.sum(sums[1], axis=0, keepdims=True) * (stretch * stretch)
        return carry

    lax.fori_loop(low, high, body, 0)


def speeds_of(norms, speeds):
    force = jnp.sum(norms[0], axis=1, keepdims=True)
    path = jnp.sum(norms[1], axis=1, keepdims=True)
    value = jnp.sqrt(force + EPSILON) / jnp.sqrt(path + EPSILON)
    speeds[...] = jnp.broadcast_to(value, speeds.shape)


def theta_pass(phi, speeds, theta, low, high, first, count, shift=0):
    tiles = phi.shape[2] // LANES

    def body(k, carry):
        before, after, stretch = neighbours_of(k, first, count)
        scale = speeds[pl.ds(k - shift, 1), :] * stretch
        for t in range(tiles):
            cols = tile_of(t)
            theta[k, :, cols] = scale * (phi[after, :, cols] - phi[before, :, cols]) - theta[k, :, cols]
        return carry

    lax.fori_loop(low, high, body, 0)


def update_pass(phi, speeds, theta, low, high, first, count, store, shift=0):
    rows = phi.shape[1]
    tiles = phi.shape[2] // LANES

    def body(k, carry):
        before, after, stretch = neighbours_of(k, first, count)
        scale = speeds[pl.ds(k - shift, 1), :] * stretch
        gid = k + first
        inside = (gid > 0) & (gid < count - 1)

        def use(t, center, total):
            cols = tile_of(t)
            value = phi[k, :, cols]
            descent = (
                scale * (theta[after, :, cols] - theta[before, :, cols])
                + total
                - (3.0 * center) * (1.0 + value * value)
            )
            store(k, t, jnp.where(inside, value + TIME_STEP * descent, value))

        sum_of_neighbours(lambda t: theta[k, :, tile_of(t)], tiles, rows, use)
        return carry

    lax.fori_loop(low, high, body, 0)


def chunk_of(q):
    return max(c for c in range(len(CHUNKS)) if CHUNKS[c] <= q)


def place(phi, at, image, edge_rows):
    rows = image.shape[0]
    phi[at, 0:rows, :] = image
    phi[at, rows:, :] = edge_rows


def inner_kernel(*refs, count):
    refs = list(refs)
    pick = lambda n: [refs.pop(0) for _ in range(n)]
    (keep,), recv = pick(1), pick(len(CHUNKS))
    near_early, near_late, edge_rows, phi, drift, norms = pick(6)
    local, rows, _ = keep.shape
    hi, lo = pair_position()
    first = hi * (PAIR * local) - LOW
    top = LOW + PAIR * local

    def own_at(part, q):
        return LOW + part * local + jnp.where(part == 0, q, local - 1 - q)

    for q in range(local):
        place(phi, own_at(lo, q), keep[q], edge_rows[q])
        place(phi, own_at(1 - lo, q), recv[chunk_of(q)][q - CHUNKS[chunk_of(q)]], edge_rows[local + q])
        low_at, high_at = LOW - 1 - q, top + q
        place(phi, jnp.where(lo == 1, low_at, high_at), near_early[q], edge_rows[2 * local + q])
        if q < near_late.shape[0]:
            place(phi, jnp.where(lo == 1, high_at, low_at), near_late[q], edge_rows[3 * local + q])
    drift_pass(phi, drift, norms, LOW - 1, top + 1, first, count, rows, LOW - 1)


def middle_inner_kernel(_, __, norms, phi, theta, new_phi, new_drift, new_norms, speeds, *, count, local, rows):
    hi, _ = pair_position()
    first = hi * (PAIR * local) - LOW
    top = LOW + PAIR * local
    speeds_of(norms, speeds)
    theta_pass(phi, speeds, theta, LOW - 1, top + 1, first, count, LOW - 1)

    def store(k, t, value):
        new_phi[k, :, tile_of(t)] = value

    update_pass(phi, speeds, theta, LOW, top, first, count, store, LOW - 1)
    new_norms[...] = jnp.zeros(new_norms.shape, F32)
    drift_pass(new_phi, new_drift, new_norms, LOW + 1, top - 1, first, count, rows)


def middle_outer_kernel(norms, near_late, far_early, far_extra, far_late, rows_late, *refs, count, local):
    phi, theta, new_phi, new_drift, new_norms, speeds = refs[5:]
    rows = near_late.shape[1]
    hi, lo = pair_position()
    first = hi * (PAIR * local) - LOW
    top = LOW + PAIR * local
    window = phi.shape[0]
    done = CHUNKS[-1]
    for q in range(done, local):
        place(phi, jnp.where(lo == 1, top + q, LOW - 1 - q), near_late[q - done], rows_late[q - done])
    for i in range(FAR):
        low_at, high_at = LOW - 1 - local - i, top + local + i
        at = FAR - 1 - i
        late, late_rows = far_late.at[at], rows_late.at[local - done + at]
        early = far_early.at[SHARED - 1 - i] if i < SHARED else far_extra.at[FAR - 1 - i]
        early_rows = rows_late.at[local - done + FAR + (SHARED - 1 - i if i < SHARED else FAR - 1 - i + SHARED)]

        @pl.when(lo == 1)
        def _():
            if high_at < window:
                place(phi, high_at, early[...], early_rows[...])
            if low_at >= 0:
                place(phi, low_at, late[...], late_rows[...])

        @pl.when(lo == 0)
        def _():
            if high_at < window:
                place(phi, high_at, late[...], late_rows[...])
            if low_at >= 0:
                place(phi, low_at, early[...], early_rows[...])

    def store(k, t, value):
        new_phi[k, :, tile_of(t)] = value

    speeds_of(norms, speeds)
    for low, high in ((1, LOW - 1), (top + 1, window - 1)):
        drift_pass(phi, theta, None, low, high, first, count, rows)
        theta_pass(phi, speeds, theta, low, high, first, count)
    for low, high in ((2, LOW), (top, window - 2)):
        update_pass(phi, speeds, theta, low, high, first, count, store)
    for low, high in ((3, LOW + 1), (top - 1, window - 3)):
        drift_pass(new_phi, new_drift, new_norms, low, high, first, count, rows)


def last_kernel(phi, _, norms, final, squares, theta, speeds, *, count, local, rows, done):
    hi, _ = pair_position()
    first = hi * (PAIR * local) - LOW
    window = phi.shape[0]
    tiles = final.shape[2] // LANES
    shift = LOW - REACH
    speeds_of(norms, speeds)
    theta_pass(phi, speeds, theta, done + 1, window - done - 1, first, count)

    def store(k, t, value):
        if t < tiles:
            final[k - shift, :, tile_of(t)] = value[0:rows]

    update_pass(phi, speeds, theta, shift, shift + final.shape[0], first, count, store)
    position = (
        lax.broadcasted_iota(jnp.int32, squares.shape, 0) * LANES
        + lax.broadcasted_iota(jnp.int32, squares.shape, 1)
    )

    def body(i, total):
        k = REACH + i
        acc = jnp.zeros((SUBLANES, LANES), F32)
        for t in range(tiles):
            diff = final[k, :, tile_of(t)] - final[k - 1, :, tile_of(t)]
            acc = acc + fold(diff * diff)
        amount = jnp.sum(jnp.sum(acc, axis=0, keepdims=True), axis=1, keepdims=True)
        return total + jnp.where(position == LOW + i + first, amount, 0.0)

    squares[...] = lax.fori_loop(0, PAIR * local, body, jnp.zeros(squares.shape, F32))


def combine_kernel(bracket, window, squares, out, *scratch, count, own):
    hi, lo = pair_position()
    part = lo if own else 1 - lo
    whole, out = out, scratch[0] if own else out
    local, _, half = out.shape
    tiles = half // LANES
    begin = hi * (PAIR * local)
    position = (
        lax.broadcasted_iota(jnp.int32, squares.shape, 0) * LANES
        + lax.broadcasted_iota(jnp.int32, squares.shape, 1)
    )
    counted = (position >= 1) & (position < count)
    segments = jnp.where(counted, jnp.sqrt(squares[...] + EPSILON), 0.0)

    def total(value):
        return jnp.sum(jnp.sum(value, axis=0, keepdims=True), axis=1, keepdims=True)

    length = total(segments)
    weights = []
    for i in range(local):
        b = bracket[i]
        j = begin + part * local + i
        arc = total(jnp.where(position <= b, segments, 0.0))
        segment = total(jnp.where(position == b + 1, segments, 0.0))
        target = length * lax.convert_element_type(j, F32) / F32(count - 1)
        weights.append((target - arc) / segment)
    for i in range(local):
        at = bracket[i] - begin + REACH
        for t in range(tiles):
            base = window[at, :, tile_of(t)]
            out[i, :, tile_of(t)] = base + weights[i] * (window[at + 1, :, tile_of(t)] - base)
    if own:
        copy_half(out, whole, lo, scratch[1])


def copy_half(half_ref, whole, part, sem):
    half = half_ref.shape[2]
    copy = pltpu.make_async_copy(half_ref, whole.at[:, :, pl.ds(pl.multiple_of(part * half, LANES), half)], sem)
    copy.start()
    copy.wait()


def finish_kernel(whole_in, other, whole, sem):
    _, lo = pair_position()
    copy_half(other, whole, 1 - lo, sem)


def per_device(path, bracket):
    local, rows, columns = path.shape
    devices = lax.axis_size("img")
    count = local * devices
    half = columns // PAIR
    wide = half + LANES
    window = LOW + PAIR * local + HIGH
    if devices & (devices - 1) or ITERS != 2 or local != 2 * ITERS or count > SUBLANES * LANES or rows % SUBLANES:
        raise ValueError("unsupported sizes")
    shape = functools.partial(jax.ShapeDtypeStruct, dtype=F32)
    block = shape((local, rows, wide))
    ahead = [(i, i + PAIR) for i in range(devices - PAIR)]
    back = [(target, source) for source, target in ahead]
    move = lambda value, up, down: lax.ppermute(
        value, "img",
        [p for p in ahead if p[0] % PAIR in up] + [p for p in back if p[0] % PAIR in down],
    )
    keep, send = call(pack_kernel, (block, block), operands=1)(path)
    ends = CHUNKS[1:] + (local,)
    recv = [swap_pairs(send[a:b]) for a, b in zip(CHUNKS, ends)]
    other_bracket = swap_pairs(bracket)
    near_early = move(keep, (1,), (0,))
    far_early = move(keep[local - SHARED :], (0,), (1,))
    near_late = [move(value, (0,), (1,)) for value in recv]
    far_late = move(jnp.concatenate(recv, axis=0)[local - FAR :], (1,), (0,))
    far_extra = move(keep[local - FAR : local - SHARED], (), (1,))
    rows_early = neighbour_rows([keep] + recv + [near_early, near_late[0]])
    rows_late = neighbour_rows([near_late[1], far_late, far_early, far_extra])
    held = shape((window, rows + 2 * EDGE, wide))
    lines = -(-window // SUBLANES) * SUBLANES
    norm_shape = shape((2, lines, LANES))
    operands = [keep] + recv + [near_early, near_late[0], rows_early]
    inside = PAIR * local + 2
    inside_lines = -(-inside // SUBLANES) * SUBLANES
    phi, drift, norms = call(
        functools.partial(inner_kernel, count=count), (held, held, shape((2, inside_lines, LANES))),
        operands=len(operands),
    )(*operands)
    norms = small_sum(norms, (1,))
    own_norms = norms[:, 1 : inside - 1]
    low_norms = lax.ppermute(own_norms, "img", ahead)
    high_norms = lax.ppermute(own_norms, "img", back)
    state = call(
        functools.partial(middle_inner_kernel, count=count, local=local, rows=rows),
        (held, held, held, held, norm_shape), scratch=[pltpu.VMEM((inside_lines, LANES), F32)],
        operands=3, aliases={0: 0, 1: 1},
    )(phi, drift, norms)
    pad = jnp.zeros((2, lines - window, LANES), F32)
    norms = jnp.concatenate([low_norms[:, PAIR * local - LOW :], own_norms, high_norms[:, :HIGH], pad], axis=1)
    operands = [norms, near_late[1], far_early, far_extra, far_late, rows_late]
    _, _, phi, drift, norms = call(
        functools.partial(middle_outer_kernel, count=count, local=local),
        (held, held, held, held, norm_shape), scratch=[pltpu.VMEM((lines, LANES), F32)],
        operands=len(operands) + len(state), aliases={len(operands) + i: i for i in range(len(state))},
    )(*operands, *state)
    scratch = [pltpu.VMEM((lines, LANES), F32)]
    norms = small_sum(norms, (1,))
    final, squares, _ = call(
        functools.partial(last_kernel, count=count, local=local, rows=rows, done=2 * (ITERS - 1)),
        (shape((PAIR * local + 2 * REACH + 1, rows, half)), shape((SUBLANES, LANES)), held),
        scratch=scratch, operands=3, aliases={1: 2},
    )(phi, drift, norms)
    steps = []
    step = 1
    while step < devices:
        steps.append(step)
        step *= 2
    squares = small_sum(squares, steps)
    half_block = (local, rows, half)
    whole = shape((local, rows, columns))
    in_smem, in_vmem, in_hbm = (pl.BlockSpec(memory_space=m) for m in (pltpu.SMEM, pltpu.VMEM, pl.ANY))
    other = swap_pairs(
        call(functools.partial(combine_kernel, count=count, own=False), shape(half_block), smem=1, operands=2)(
            other_bracket, final, squares
        )
    )
    mine = pl.pallas_call(
        functools.partial(combine_kernel, count=count, own=True),
        out_shape=whole,
        in_specs=[in_smem, in_vmem, in_vmem],
        out_specs=in_hbm,
        scratch_shapes=[pltpu.VMEM(half_block, F32), pltpu.SemaphoreType.DMA],
        compiler_params=pltpu.CompilerParams(vmem_limit_bytes=VMEM_LIMIT),
    )(bracket, final, squares)
    return pl.pallas_call(
        finish_kernel,
        out_shape=whole,
        in_specs=[in_hbm, in_vmem],
        out_specs=in_hbm,
        scratch_shapes=[pltpu.SemaphoreType.DMA],
        input_output_aliases={0: 0},
        compiler_params=pltpu.CompilerParams(vmem_limit_bytes=VMEM_LIMIT),
    )(mine, other)


def solution(mesh):
    return jax.shard_map(
        per_device,
        mesh=mesh,
        in_specs=(P(("groups", "img"), "space", None), P(("groups", "img"))),
        out_specs=P(("groups", "img"), "space", None),
        check_vma=False,
    )
```

```python
import functools

import jax
import jax.numpy as jnp
from jax import lax
from jax.experimental import pallas as pl
from jax.experimental.pallas import tpu as pltpu
from jax.sharding import PartitionSpec as P


REACH = 2
ITERS = 2
TIME_STEP = 0.002
EPSILON = 1e-06

LANES = 128
SUBLANES = 8
PAIR = 2
LOW = 2 * ITERS + REACH
HIGH = 2 * ITERS + REACH + 1
FAR = 3
SHARED = 2
EDGE = 2 * ITERS
CHUNKS = (0, 2)
VMEM_LIMIT = 4 * 1024 * 1024

F32 = jnp.float32


def call(kernel, out_shapes, scratch=(), smem=0, operands=0, aliases=None):
    specs = [pl.BlockSpec(memory_space=pltpu.SMEM)] * smem
    specs += [pl.BlockSpec(memory_space=pltpu.VMEM)] * operands
    return pl.pallas_call(
        kernel,
        out_shape=out_shapes,
        in_specs=specs,
        out_specs=jax.tree.map(lambda _: pl.BlockSpec(memory_space=pltpu.VMEM), out_shapes),
        scratch_shapes=list(scratch),
        input_output_aliases=aliases or {},
        compiler_params=pltpu.CompilerParams(vmem_limit_bytes=VMEM_LIMIT),
    )


def pair_position():
    index = lax.axis_index("img")
    return lax.div(index, PAIR), lax.rem(index, PAIR)


def swap_pairs(value):
    count = lax.axis_size("img")
    return lax.ppermute(value, "img", [(i, i ^ 1) for i in range(count)])


def small_sum(value, steps):
    size = lax.axis_size("space")
    if size & (size - 1) == 0:
        step = 1
        while step < size:
            value = value + lax.ppermute(value, "space", [(i, i ^ step) for i in range(size)])
            step *= 2
    else:
        value = lax.psum(value, "space")
    count = lax.axis_size("img")
    for step in steps:
        value = value + lax.ppermute(value, "img", [(i, i ^ step) for i in range(count)])
    return value


def tile_of(t):
    return slice(t * LANES, (t + 1) * LANES)


def images_of(message, tiles):
    return (message.shape[0] - 1) // tiles


def edge_tile(message, i):
    return pltpu.roll(message[message.shape[0] - 1], LANES - EDGE - 2 * EDGE * i, 1)


def pack_edges(tiles):
    lane = lax.broadcasted_iota(jnp.int32, tiles[0].shape, 1)
    packed = jnp.zeros(tiles[0].shape, F32)
    for i, tile in enumerate(tiles):
        mine = (lane >= 2 * EDGE * i) & (lane < 2 * EDGE * (i + 1))
        packed = jnp.where(mine, pltpu.roll(tile, EDGE + 2 * EDGE * i, 1), packed)
    return packed


def pick_kernel(*refs):
    *messages, picked = refs
    tiles = picked.shape[2] // LANES - 1
    at = 0
    for message in messages:
        for i in range(images_of(message, tiles)):
            for t in range(tiles + 1):
                tile = message[i * tiles + t] if t < tiles else edge_tile(message, i)
                picked[at, 0:EDGE, tile_of(t)] = tile[0:EDGE]
                picked[at, EDGE:, tile_of(t)] = tile[tile.shape[0] - EDGE :]
            at += 1


def neighbour_rows(tiles, blocks):
    size = lax.axis_size("space")
    count = sum(images_of(block, tiles) for block in blocks)
    picked = call(
        pick_kernel, jax.ShapeDtypeStruct((count, 2 * EDGE, (tiles + 1) * LANES), F32), operands=len(blocks)
    )(*blocks)
    if size == 1:
        return picked
    if size == 2:
        return lax.ppermute(picked, "space", [(0, 1), (1, 0)])
    after = lax.ppermute(picked[:, :EDGE], "space", [(i, (i - 1) % size) for i in range(size)])
    before = lax.ppermute(picked[:, EDGE:], "space", [(i, (i + 1) % size) for i in range(size)])
    return jnp.concatenate([after, before], axis=1)


def pack_kernel(x_ref, keep_ref, send_first, send_second, shared_ref, extra_ref):
    _, lo = pair_position()
    local, rows, columns = x_ref.shape
    half = columns // PAIR
    tiles = half // LANES
    lane = lax.broadcasted_iota(jnp.int32, (rows, LANES), 1)

    def fill(ref, part, chosen):
        begin = part * half
        right = pl.multiple_of((1 - part) * half, LANES)
        left = pl.multiple_of((1 - part) * half + half - LANES, LANES)
        edges = []
        for i, q in enumerate(chosen):
            k = jnp.where(lo == 0, q, local - 1 - q)
            for t in range(tiles):
                ref[i * tiles + t] = x_ref[k, :, pl.ds(pl.multiple_of(begin + t * LANES, LANES), LANES)]
            edges.append(
                jnp.where(lane < LANES // 2, x_ref[k, :, pl.ds(right, LANES)], x_ref[k, :, pl.ds(left, LANES)])
            )
        ref[len(chosen) * tiles] = pack_edges(edges)

    fill(send_first, 1 - lo, range(CHUNKS[1]))
    fill(send_second, 1 - lo, range(CHUNKS[1], local))
    fill(keep_ref, lo, range(local))
    fill(shared_ref, lo, range(local - SHARED, local))
    fill(extra_ref, lo, range(local - FAR, local - SHARED))


def far_kernel(first, second, out):
    tiles = (first.shape[0] - 1) // CHUNKS[1]
    local = CHUNKS[1] + images_of(second, tiles)
    edges = []
    for i, q in enumerate(range(local - FAR, local)):
        source, at = (first, q) if q < CHUNKS[1] else (second, q - CHUNKS[1])
        for t in range(tiles):
            out[i * tiles + t] = source[at * tiles + t]
        edges.append(edge_tile(source, at))
    out[FAR * tiles] = pack_edges(edges)


def sum_of_neighbours(load, tiles, rows, use):
    lane = lax.broadcasted_iota(jnp.int32, (rows, LANES), 1)
    is_first, is_last = lane == 0, lane == LANES - 1
    center = load(0)
    from_left = pltpu.roll(load(tiles - 1), 1, 1)
    to_left = pltpu.roll(center, LANES - 1, 1)
    for t in range(tiles):
        following = load((t + 1) % tiles)
        shifted = pltpu.roll(center, 1, 1)
        next_to_left = pltpu.roll(following, LANES - 1, 1)
        west = jnp.where(is_first, from_left, shifted)
        east = jnp.where(is_last, next_to_left, to_left)
        north = pltpu.roll(center, 1, 0)
        south = pltpu.roll(center, rows - 1, 0)
        use(t, center, (north + south) + (west + east))
        center, from_left, to_left = following, shifted, next_to_left


def neighbours_of(k, first, count):
    gid = k + first
    is_first, is_last = gid == 0, gid == count - 1
    before = jnp.where(is_first, k, k - 1)
    after = jnp.where(is_last, k, k + 1)
    stretch = jnp.where(is_first | is_last, F32(count - 1), F32((count - 1) / 2.0))
    return before, after, stretch


def fold(value):
    return jnp.sum(value.reshape(-1, SUBLANES, LANES), axis=0)


def drift_pass(phi, drift, norms, low, high, first, count, own_rows, shift=0):
    rows = phi.shape[1]
    tiles = phi.shape[2] // LANES

    def body(k, carry):
        before, after, stretch = neighbours_of(k, first, count)
        sums = [jnp.zeros((SUBLANES, LANES), F32), jnp.zeros((SUBLANES, LANES), F32)]

        def use(t, center, total):
            force = total - center * (3.0 + center * center)
            drift[k, :, tile_of(t)] = force
            if t < tiles - 1 and norms is not None:
                step = phi[after, 0:own_rows, tile_of(t)] - phi[before, 0:own_rows, tile_of(t)]
                own = force[0:own_rows]
                sums[0] = sums[0] + fold(own * own)
                sums[1] = sums[1] + fold(step * step)

        sum_of_neighbours(lambda t: phi[k, :, tile_of(t)], tiles, rows, use)
        if norms is not None:
            norms[0, pl.ds(k - shift, 1), :] = jnp.sum(sums[0], axis=0, keepdims=True)
            norms[1, pl.ds(k - shift, 1), :] = jnp.sum(sums[1], axis=0, keepdims=True) * (stretch * stretch)
        return carry

    lax.fori_loop(low, high, body, 0)


def speeds_of(norms, speeds):
    force = jnp.sum(norms[0], axis=1, keepdims=True)
    path = jnp.sum(norms[1], axis=1, keepdims=True)
    value = jnp.sqrt(force + EPSILON) / jnp.sqrt(path + EPSILON)
    speeds[...] = jnp.broadcast_to(value, speeds.shape)


def theta_pass(phi, speeds, theta, low, high, first, count, shift=0):
    tiles = phi.shape[2] // LANES

    def body(k, carry):
        before, after, stretch = neighbours_of(k, first, count)
        scale = speeds[pl.ds(k - shift, 1), :] * stretch
        for t in range(tiles):
            cols = tile_of(t)
            theta[k, :, cols] = scale * (phi[after, :, cols] - phi[before, :, cols]) - theta[k, :, cols]
        return carry

    lax.fori_loop(low, high, body, 0)


def update_pass(phi, speeds, theta, low, high, first, count, store, shift=0):
    rows = phi.shape[1]
    tiles = phi.shape[2] // LANES

    def body(k, carry):
        before, after, stretch = neighbours_of(k, first, count)
        scale = speeds[pl.ds(k - shift, 1), :] * stretch
        gid = k + first
        inside = (gid > 0) & (gid < count - 1)

        def use(t, center, total):
            cols = tile_of(t)
            value = phi[k, :, cols]
            descent = (
                scale * (theta[after, :, cols] - theta[before, :, cols])
                + total
                - (3.0 * center) * (1.0 + value * value)
            )
            store(k, t, jnp.where(inside, value + TIME_STEP * descent, value))

        sum_of_neighbours(lambda t: theta[k, :, tile_of(t)], tiles, rows, use)
        return carry

    lax.fori_loop(low, high, body, 0)


def place(phi, at, message, i, edge_rows):
    rows = message.shape[1]
    tiles = phi.shape[2] // LANES - 1
    for t in range(tiles):
        phi[at, 0:rows, tile_of(t)] = message[i * tiles + t]
    phi[at, 0:rows, tile_of(tiles)] = edge_tile(message, i)
    phi[at, rows:, :] = edge_rows


def inner_kernel(*refs, count, local):
    keep, first_recv, second_recv, near_early, near_late, edge_rows, phi, drift, norms = refs
    rows = keep.shape[1]
    hi, lo = pair_position()
    first = hi * (PAIR * local) - LOW
    top = LOW + PAIR * local
    half = CHUNKS[1]

    def own_at(part, q):
        return LOW + part * local + jnp.where(part == 0, q, local - 1 - q)

    for q in range(local):
        place(phi, own_at(lo, q), keep, q, edge_rows[q])
        source, at = (first_recv, q) if q < half else (second_recv, q - half)
        place(phi, own_at(1 - lo, q), source, at, edge_rows[local + q])
        low_at, high_at = LOW - 1 - q, top + q
        place(phi, jnp.where(lo == 1, low_at, high_at), near_early, q, edge_rows[2 * local + q])
        if q < half:
            place(phi, jnp.where(lo == 1, high_at, low_at), near_late, q, edge_rows[3 * local + q])
    drift_pass(phi, drift, norms, LOW - 1, top + 1, first, count, rows, LOW - 1)


def middle_inner_kernel(_, __, norms, phi, theta, new_phi, new_drift, new_norms, speeds, *, count, local, rows):
    hi, _ = pair_position()
    first = hi * (PAIR * local) - LOW
    top = LOW + PAIR * local
    speeds_of(norms, speeds)
    theta_pass(phi, speeds, theta, LOW - 1, top + 1, first, count, LOW - 1)

    def store(k, t, value):
        new_phi[k, :, tile_of(t)] = value

    update_pass(phi, speeds, theta, LOW, top, first, count, store, LOW - 1)
    new_norms[...] = jnp.zeros(new_norms.shape, F32)
    drift_pass(new_phi, new_drift, new_norms, LOW + 1, top - 1, first, count, rows)


def middle_outer_kernel(norms, near_late, far_early, far_extra, far_late, rows_late, *refs, count, local):
    phi, theta, new_phi, new_drift, new_norms, speeds = refs[5:]
    rows = near_late.shape[1]
    hi, lo = pair_position()
    first = hi * (PAIR * local) - LOW
    top = LOW + PAIR * local
    window = phi.shape[0]
    done = CHUNKS[-1]
    for q in range(done, local):
        place(phi, jnp.where(lo == 1, top + q, LOW - 1 - q), near_late, q - done, rows_late[q - done])
    for i in range(FAR):
        low_at, high_at = LOW - 1 - local - i, top + local + i
        at = FAR - 1 - i
        late = (far_late, at, rows_late.at[local - done + at])
        if i < SHARED:
            early = (far_early, SHARED - 1 - i, rows_late.at[local - done + FAR + SHARED - 1 - i])
        else:
            early = (far_extra, FAR - 1 - i, rows_late.at[local - done + FAR + FAR - 1 - i + SHARED])

        @pl.when(lo == 1)
        def _():
            for position, (message, index, edge) in ((high_at, early), (low_at, late)):
                if 0 <= position < window:
                    place(phi, position, message, index, edge[...])

        @pl.when(lo == 0)
        def _():
            for position, (message, index, edge) in ((high_at, late), (low_at, early)):
                if 0 <= position < window:
                    place(phi, position, message, index, edge[...])

    def store(k, t, value):
        new_phi[k, :, tile_of(t)] = value

    speeds_of(norms, speeds)
    for low, high in ((1, LOW - 1), (top + 1, window - 1)):
        drift_pass(phi, theta, None, low, high, first, count, rows)
        theta_pass(phi, speeds, theta, low, high, first, count)
    for low, high in ((2, LOW), (top, window - 2)):
        update_pass(phi, speeds, theta, low, high, first, count, store)
    for low, high in ((3, LOW + 1), (top - 1, window - 3)):
        drift_pass(new_phi, new_drift, new_norms, low, high, first, count, rows)


def last_kernel(phi, _, norms, final, squares, theta, speeds, *, count, local, rows, done):
    hi, _ = pair_position()
    first = hi * (PAIR * local) - LOW
    window = phi.shape[0]
    tiles = final.shape[2] // LANES
    shift = LOW - REACH
    speeds_of(norms, speeds)
    theta_pass(phi, speeds, theta, done + 1, window - done - 1, first, count)

    def store(k, t, value):
        if t < tiles:
            final[k - shift, :, tile_of(t)] = value[0:rows]

    update_pass(phi, speeds, theta, shift, shift + final.shape[0], first, count, store)
    position = (
        lax.broadcasted_iota(jnp.int32, squares.shape, 0) * LANES
        + lax.broadcasted_iota(jnp.int32, squares.shape, 1)
    )

    def body(i, total):
        k = REACH + i
        acc = jnp.zeros((SUBLANES, LANES), F32)
        for t in range(tiles):
            diff = final[k, :, tile_of(t)] - final[k - 1, :, tile_of(t)]
            acc = acc + fold(diff * diff)
        amount = jnp.sum(jnp.sum(acc, axis=0, keepdims=True), axis=1, keepdims=True)
        return total + jnp.where(position == LOW + i + first, amount, 0.0)

    squares[...] = lax.fori_loop(0, PAIR * local, body, jnp.zeros(squares.shape, F32))


def combine_kernel(bracket, window, squares, out, *scratch, count, own):
    hi, lo = pair_position()
    part = lo if own else 1 - lo
    whole, out = out, scratch[0] if own else out
    local, _, half = out.shape
    tiles = half // LANES
    begin = hi * (PAIR * local)
    position = (
        lax.broadcasted_iota(jnp.int32, squares.shape, 0) * LANES
        + lax.broadcasted_iota(jnp.int32, squares.shape, 1)
    )
    counted = (position >= 1) & (position < count)
    segments = jnp.where(counted, jnp.sqrt(squares[...] + EPSILON), 0.0)

    def total(value):
        return jnp.sum(jnp.sum(value, axis=0, keepdims=True), axis=1, keepdims=True)

    length = total(segments)
    weights = []
    for i in range(local):
        b = bracket[i]
        j = begin + part * local + i
        arc = total(jnp.where(position <= b, segments, 0.0))
        segment = total(jnp.where(position == b + 1, segments, 0.0))
        target = length * lax.convert_element_type(j, F32) / F32(count - 1)
        weights.append((target - arc) / segment)
    for i in range(local):
        at = bracket[i] - begin + REACH
        for t in range(tiles):
            base = window[at, :, tile_of(t)]
            out[i, :, tile_of(t)] = base + weights[i] * (window[at + 1, :, tile_of(t)] - base)
    if own:
        copy_half(out, whole, lo, scratch[1])


def copy_half(half_ref, whole, part, sem):
    half = half_ref.shape[2]
    copy = pltpu.make_async_copy(half_ref, whole.at[:, :, pl.ds(pl.multiple_of(part * half, LANES), half)], sem)
    copy.start()
    copy.wait()


def finish_kernel(whole_in, other, whole, sem):
    _, lo = pair_position()
    copy_half(other, whole, 1 - lo, sem)


def per_device(path, bracket):
    local, rows, columns = path.shape
    devices = lax.axis_size("img")
    count = local * devices
    half = columns // PAIR
    wide = half + LANES
    window = LOW + PAIR * local + HIGH
    if devices & (devices - 1) or ITERS != 2 or local != 2 * ITERS or count > SUBLANES * LANES or rows % SUBLANES:
        raise ValueError("unsupported sizes")
    shape = functools.partial(jax.ShapeDtypeStruct, dtype=F32)
    ahead = [(i, i + PAIR) for i in range(devices - PAIR)]
    back = [(target, source) for source, target in ahead]
    move = lambda value, up, down: lax.ppermute(
        value, "img",
        [p for p in ahead if p[0] % PAIR in up] + [p for p in back if p[0] % PAIR in down],
    )
    tiles = half // LANES
    message = lambda n: shape((n * tiles + 1, rows, LANES))
    first_chunk = CHUNKS[1]
    keep, send_first, send_second, shared, extra = call(
        pack_kernel,
        (message(local), message(first_chunk), message(local - first_chunk), message(SHARED), message(FAR - SHARED)),
        operands=1,
    )(path)
    recv = [swap_pairs(send_first), swap_pairs(send_second)]
    other_bracket = swap_pairs(bracket)
    near_early = move(keep, (1,), (0,))
    far_early = move(shared, (0,), (1,))
    near_late = [move(value, (0,), (1,)) for value in recv]
    far_late = move(call(far_kernel, message(FAR), operands=2)(*recv), (1,), (0,))
    far_extra = move(extra, (), (1,))
    rows_early = neighbour_rows(tiles, [keep] + recv + [near_early, near_late[0]])
    rows_late = neighbour_rows(tiles, [near_late[1], far_late, far_early, far_extra])
    held = shape((window, rows + 2 * EDGE, wide))
    lines = -(-window // SUBLANES) * SUBLANES
    norm_shape = shape((2, lines, LANES))
    operands = [keep] + recv + [near_early, near_late[0], rows_early]
    inside = PAIR * local + 2
    inside_lines = -(-inside // SUBLANES) * SUBLANES
    phi, drift, norms = call(
        functools.partial(inner_kernel, count=count, local=local), (held, held, shape((2, inside_lines, LANES))),
        operands=len(operands),
    )(*operands)
    norms = small_sum(norms, (1,))
    own_norms = norms[:, 1 : inside - 1]
    low_norms = lax.ppermute(own_norms, "img", ahead)
    high_norms = lax.ppermute(own_norms, "img", back)
    state = call(
        functools.partial(middle_inner_kernel, count=count, local=local, rows=rows),
        (held, held, held, held, norm_shape), scratch=[pltpu.VMEM((inside_lines, LANES), F32)],
        operands=3, aliases={0: 0, 1: 1},
    )(phi, drift, norms)
    pad = jnp.zeros((2, lines - window, LANES), F32)
    norms = jnp.concatenate([low_norms[:, PAIR * local - LOW :], own_norms, high_norms[:, :HIGH], pad], axis=1)
    operands = [norms, near_late[1], far_early, far_extra, far_late, rows_late]
    _, _, phi, drift, norms = call(
        functools.partial(middle_outer_kernel, count=count, local=local),
        (held, held, held, held, norm_shape), scratch=[pltpu.VMEM((lines, LANES), F32)],
        operands=len(operands) + len(state), aliases={len(operands) + i: i for i in range(len(state))},
    )(*operands, *state)
    scratch = [pltpu.VMEM((lines, LANES), F32)]
    norms = small_sum(norms, (1,))
    final, squares, _ = call(
        functools.partial(last_kernel, count=count, local=local, rows=rows, done=2 * (ITERS - 1)),
        (shape((PAIR * local + 2 * REACH + 1, rows, half)), shape((SUBLANES, LANES)), held),
        scratch=scratch, operands=3, aliases={1: 2},
    )(phi, drift, norms)
    steps = []
    step = 1
    while step < devices:
        steps.append(step)
        step *= 2
    squares = small_sum(squares, steps)
    half_block = (local, rows, half)
    whole = shape((local, rows, columns))
    in_smem, in_vmem, in_hbm = (pl.BlockSpec(memory_space=m) for m in (pltpu.SMEM, pltpu.VMEM, pl.ANY))
    other = swap_pairs(
        call(functools.partial(combine_kernel, count=count, own=False), shape(half_block), smem=1, operands=2)(
            other_bracket, final, squares
        )
    )
    mine = pl.pallas_call(
        functools.partial(combine_kernel, count=count, own=True),
        out_shape=whole,
        in_specs=[in_smem, in_vmem, in_vmem],
        out_specs=in_hbm,
        scratch_shapes=[pltpu.VMEM(half_block, F32), pltpu.SemaphoreType.DMA],
        compiler_params=pltpu.CompilerParams(vmem_limit_bytes=VMEM_LIMIT),
    )(bracket, final, squares)
    return pl.pallas_call(
        finish_kernel,
        out_shape=whole,
        in_specs=[in_hbm, in_vmem],
        out_specs=in_hbm,
        scratch_shapes=[pltpu.SemaphoreType.DMA],
        input_output_aliases={0: 0},
        compiler_params=pltpu.CompilerParams(vmem_limit_bytes=VMEM_LIMIT),
    )(mine, other)


def solution(mesh):
    return jax.shard_map(
        per_device,
        mesh=mesh,
        in_specs=(P(("groups", "img"), "space", None), P(("groups", "img"))),
        out_specs=P(("groups", "img"), "space", None),
        check_vma=False,
    )
```

```python
import functools

import jax
import jax.numpy as jnp
from jax import lax
from jax.experimental import pallas as pl
from jax.experimental.pallas import tpu as pltpu
from jax.sharding import PartitionSpec as P


REACH = 2
ITERS = 2
TIME_STEP = 0.002
EPSILON = 1e-06

LANES = 128
SUBLANES = 8
PAIR = 2
LOW = 2 * ITERS + REACH
HIGH = 2 * ITERS + REACH + 1
FAR = 3
SHARED = 2
EDGE = 2 * ITERS
CHUNKS = (0, 2)
VMEM_LIMIT = 4 * 1024 * 1024

F32 = jnp.float32


def call(kernel, out_shapes, scratch=(), smem=0, operands=0, aliases=None):
    specs = [pl.BlockSpec(memory_space=pltpu.SMEM)] * smem
    specs += [pl.BlockSpec(memory_space=pltpu.VMEM)] * operands
    return pl.pallas_call(
        kernel,
        out_shape=out_shapes,
        in_specs=specs,
        out_specs=jax.tree.map(lambda _: pl.BlockSpec(memory_space=pltpu.VMEM), out_shapes),
        scratch_shapes=list(scratch),
        input_output_aliases=aliases or {},
        compiler_params=pltpu.CompilerParams(vmem_limit_bytes=VMEM_LIMIT),
    )


def pair_position():
    index = lax.axis_index("img")
    return lax.div(index, PAIR), lax.rem(index, PAIR)


def swap_pairs(value):
    count = lax.axis_size("img")
    return lax.ppermute(value, "img", [(i, i ^ 1) for i in range(count)])


def small_sum(value, steps):
    size = lax.axis_size("space")
    if size & (size - 1) == 0:
        step = 1
        while step < size:
            value = value + lax.ppermute(value, "space", [(i, i ^ step) for i in range(size)])
            step *= 2
    else:
        value = lax.psum(value, "space")
    count = lax.axis_size("img")
    for step in steps:
        other = lax.ppermute(value, "img", [(i, i ^ step) for i in range(count)])
        value = value + other
    return value


def tile_of(t):
    return slice(t * LANES, (t + 1) * LANES)


def images_of(message, tiles):
    return (message.shape[0] - 1) // tiles


def edge_tile(message, i):
    return pltpu.roll(message[message.shape[0] - 1], LANES - EDGE - 2 * EDGE * i, 1)


def pack_edges(tiles):
    lane = lax.broadcasted_iota(jnp.int32, tiles[0].shape, 1)
    packed = jnp.zeros(tiles[0].shape, F32)
    for i, tile in enumerate(tiles):
        mine = (lane >= 2 * EDGE * i) & (lane < 2 * EDGE * (i + 1))
        packed = jnp.where(mine, pltpu.roll(tile, EDGE + 2 * EDGE * i, 1), packed)
    return packed


def pick_kernel(*refs):
    *messages, picked = refs
    tiles = picked.shape[2] // LANES - 1
    at = 0
    for message in messages:
        for i in range(images_of(message, tiles)):
            for t in range(tiles + 1):
                tile = message[i * tiles + t] if t < tiles else edge_tile(message, i)
                picked[at, 0:EDGE, tile_of(t)] = tile[0:EDGE]
                picked[at, EDGE:, tile_of(t)] = tile[tile.shape[0] - EDGE :]
            at += 1


def neighbour_rows(tiles, blocks):
    size = lax.axis_size("space")
    count = sum(images_of(block, tiles) for block in blocks)
    picked = call(
        pick_kernel, jax.ShapeDtypeStruct((count, 2 * EDGE, (tiles + 1) * LANES), F32), operands=len(blocks)
    )(*blocks)
    if size == 1:
        return picked
    if size == 2:
        return lax.ppermute(picked, "space", [(0, 1), (1, 0)])
    after = lax.ppermute(picked[:, :EDGE], "space", [(i, (i - 1) % size) for i in range(size)])
    before = lax.ppermute(picked[:, EDGE:], "space", [(i, (i + 1) % size) for i in range(size)])
    return jnp.concatenate([after, before], axis=1)


def pack_kernel(x_ref, keep_ref, send_first, send_second, shared_ref, extra_ref):
    _, lo = pair_position()
    local, rows, columns = x_ref.shape
    half = columns // PAIR
    tiles = half // LANES
    lane = lax.broadcasted_iota(jnp.int32, (rows, LANES), 1)

    def fill(ref, part, chosen):
        begin = part * half
        right = pl.multiple_of((1 - part) * half, LANES)
        left = pl.multiple_of((1 - part) * half + half - LANES, LANES)
        edges = []
        for i, q in enumerate(chosen):
            k = jnp.where(lo == 0, q, local - 1 - q)
            for t in range(tiles):
                ref[i * tiles + t] = x_ref[k, :, pl.ds(pl.multiple_of(begin + t * LANES, LANES), LANES)]
            edges.append(
                jnp.where(lane < LANES // 2, x_ref[k, :, pl.ds(right, LANES)], x_ref[k, :, pl.ds(left, LANES)])
            )
        ref[len(chosen) * tiles] = pack_edges(edges)

    fill(send_first, 1 - lo, range(CHUNKS[1]))
    fill(send_second, 1 - lo, range(CHUNKS[1], local))
    fill(keep_ref, lo, range(local))
    fill(shared_ref, lo, range(local - SHARED, local))
    fill(extra_ref, lo, range(local - FAR, local - SHARED))


def far_kernel(first, second, out):
    tiles = (first.shape[0] - 1) // CHUNKS[1]
    local = CHUNKS[1] + images_of(second, tiles)
    edges = []
    for i, q in enumerate(range(local - FAR, local)):
        source, at = (first, q) if q < CHUNKS[1] else (second, q - CHUNKS[1])
        for t in range(tiles):
            out[i * tiles + t] = source[at * tiles + t]
        edges.append(edge_tile(source, at))
    out[FAR * tiles] = pack_edges(edges)


def sum_of_neighbours(load, tiles, rows, use):
    lane = lax.broadcasted_iota(jnp.int32, (rows, LANES), 1)
    is_first, is_last = lane == 0, lane == LANES - 1
    center = load(0)
    from_left = pltpu.roll(load(tiles - 1), 1, 1)
    to_left = pltpu.roll(center, LANES - 1, 1)
    for t in range(tiles):
        following = load((t + 1) % tiles)
        shifted = pltpu.roll(center, 1, 1)
        next_to_left = pltpu.roll(following, LANES - 1, 1)
        west = jnp.where(is_first, from_left, shifted)
        east = jnp.where(is_last, next_to_left, to_left)
        north = pltpu.roll(center, 1, 0)
        south = pltpu.roll(center, rows - 1, 0)
        use(t, center, (north + south) + (west + east))
        center, from_left, to_left = following, shifted, next_to_left


def neighbours_of(k, first, count):
    gid = k + first
    is_first, is_last = gid == 0, gid == count - 1
    before = jnp.where(is_first, k, k - 1)
    after = jnp.where(is_last, k, k + 1)
    stretch = jnp.where(is_first | is_last, F32(count - 1), F32((count - 1) / 2.0))
    return before, after, stretch


def fold(value):
    return jnp.sum(value.reshape(-1, SUBLANES, LANES), axis=0)


def drift_pass(phi, drift, norms, low, high, first, count, own_rows, shift=0):
    rows = phi.shape[1]
    tiles = phi.shape[2] // LANES

    def body(k, carry):
        before, after, stretch = neighbours_of(k, first, count)
        sums = [jnp.zeros((SUBLANES, LANES), F32), jnp.zeros((SUBLANES, LANES), F32)]

        def use(t, center, total):
            force = total - center * (3.0 + center * center)
            drift[k, :, tile_of(t)] = force
            if t < tiles - 1 and norms is not None:
                step = phi[after, 0:own_rows, tile_of(t)] - phi[before, 0:own_rows, tile_of(t)]
                own = force[0:own_rows]
                sums[0] = sums[0] + fold(own * own)
                sums[1] = sums[1] + fold(step * step)

        sum_of_neighbours(lambda t: phi[k, :, tile_of(t)], tiles, rows, use)
        if norms is not None:
            norms[0, pl.ds(k - shift, 1), :] = jnp.sum(sums[0], axis=0, keepdims=True)
            norms[1, pl.ds(k - shift, 1), :] = jnp.sum(sums[1], axis=0, keepdims=True) * (stretch * stretch)
        return carry

    lax.fori_loop(low, high, body, 0)


def speeds_of(norms, speeds):
    force = jnp.sum(norms[0], axis=1, keepdims=True)
    path = jnp.sum(norms[1], axis=1, keepdims=True)
    value = jnp.sqrt(force + EPSILON) / jnp.sqrt(path + EPSILON)
    speeds[...] = jnp.broadcast_to(value, speeds.shape)


def theta_pass(phi, speeds, theta, low, high, first, count, shift=0):
    tiles = phi.shape[2] // LANES

    def body(k, carry):
        before, after, stretch = neighbours_of(k, first, count)
        scale = speeds[pl.ds(k - shift, 1), :] * stretch
        for t in range(tiles):
            cols = tile_of(t)
            theta[k, :, cols] = scale * (phi[after, :, cols] - phi[before, :, cols]) - theta[k, :, cols]
        return carry

    lax.fori_loop(low, high, body, 0)


def update_pass(phi, speeds, theta, low, high, first, count, store, shift=0):
    rows = phi.shape[1]
    tiles = phi.shape[2] // LANES

    def body(k, carry):
        before, after, stretch = neighbours_of(k, first, count)
        scale = speeds[pl.ds(k - shift, 1), :] * stretch
        gid = k + first
        inside = (gid > 0) & (gid < count - 1)

        def use(t, center, total):
            cols = tile_of(t)
            value = phi[k, :, cols]
            descent = (
                scale * (theta[after, :, cols] - theta[before, :, cols])
                + total
                - (3.0 * center) * (1.0 + value * value)
            )
            store(k, t, jnp.where(inside, value + TIME_STEP * descent, value))

        sum_of_neighbours(lambda t: theta[k, :, tile_of(t)], tiles, rows, use)
        return carry

    lax.fori_loop(low, high, body, 0)


def place(phi, at, message, i, edge_rows):
    rows = message.shape[1]
    tiles = phi.shape[2] // LANES - 1
    for t in range(tiles):
        phi[at, 0:rows, tile_of(t)] = message[i * tiles + t]
    phi[at, 0:rows, tile_of(tiles)] = edge_tile(message, i)
    phi[at, rows:, :] = edge_rows


def inner_kernel(*refs, count, local):
    keep, first_recv, second_recv, near_early, near_late, edge_rows, phi, drift, norms = refs
    rows = keep.shape[1]
    hi, lo = pair_position()
    first = hi * (PAIR * local) - LOW
    top = LOW + PAIR * local
    half = CHUNKS[1]

    def own_at(part, q):
        return LOW + part * local + jnp.where(part == 0, q, local - 1 - q)

    for q in range(local):
        place(phi, own_at(lo, q), keep, q, edge_rows[q])
        source, at = (first_recv, q) if q < half else (second_recv, q - half)
        place(phi, own_at(1 - lo, q), source, at, edge_rows[local + q])
        low_at, high_at = LOW - 1 - q, top + q
        place(phi, jnp.where(lo == 1, low_at, high_at), near_early, q, edge_rows[2 * local + q])
        if q < half:
            place(phi, jnp.where(lo == 1, high_at, low_at), near_late, q, edge_rows[3 * local + q])
    drift_pass(phi, drift, norms, LOW - 1, top + 1, first, count, rows, LOW - 1)


def middle_inner_kernel(_, __, norms, phi, theta, new_phi, new_drift, new_norms, speeds, *, count, local, rows):
    hi, _ = pair_position()
    first = hi * (PAIR * local) - LOW
    top = LOW + PAIR * local
    speeds_of(norms, speeds)
    theta_pass(phi, speeds, theta, LOW - 1, top + 1, first, count, LOW - 1)

    def store(k, t, value):
        new_phi[k, :, tile_of(t)] = value

    update_pass(phi, speeds, theta, LOW, top, first, count, store, LOW - 1)
    new_norms[...] = jnp.zeros(new_norms.shape, F32)
    drift_pass(new_phi, new_drift, new_norms, LOW + 1, top - 1, first, count, rows)


def middle_outer_kernel(norms, near_late, far_early, far_extra, far_late, rows_late, *refs, count, local):
    phi, theta, new_phi, new_drift, new_norms, speeds = refs[5:]
    rows = near_late.shape[1]
    hi, lo = pair_position()
    first = hi * (PAIR * local) - LOW
    top = LOW + PAIR * local
    window = phi.shape[0]
    done = CHUNKS[-1]
    for q in range(done, local):
        place(phi, jnp.where(lo == 1, top + q, LOW - 1 - q), near_late, q - done, rows_late[q - done])
    for i in range(FAR):
        low_at, high_at = LOW - 1 - local - i, top + local + i
        at = FAR - 1 - i
        late = (far_late, at, rows_late.at[local - done + at])
        if i < SHARED:
            early = (far_early, SHARED - 1 - i, rows_late.at[local - done + FAR + SHARED - 1 - i])
        else:
            early = (far_extra, FAR - 1 - i, rows_late.at[local - done + FAR + FAR - 1 - i + SHARED])

        @pl.when(lo == 1)
        def _():
            for position, (message, index, edge) in ((high_at, early), (low_at, late)):
                if 0 <= position < window:
                    place(phi, position, message, index, edge[...])

        @pl.when(lo == 0)
        def _():
            for position, (message, index, edge) in ((high_at, late), (low_at, early)):
                if 0 <= position < window:
                    place(phi, position, message, index, edge[...])

    def store(k, t, value):
        new_phi[k, :, tile_of(t)] = value

    speeds_of(norms, speeds)
    for low, high in ((1, LOW - 1), (top + 1, window - 1)):
        drift_pass(phi, theta, None, low, high, first, count, rows)
        theta_pass(phi, speeds, theta, low, high, first, count)
    for low, high in ((2, LOW), (top, window - 2)):
        update_pass(phi, speeds, theta, low, high, first, count, store)
    for low, high in ((3, LOW + 1), (top - 1, window - 3)):
        drift_pass(new_phi, new_drift, new_norms, low, high, first, count, rows)


def last_kernel(phi, _, norms, final, squares, theta, speeds, *, count, local, rows):
    hi, _ = pair_position()
    first = hi * (PAIR * local) - LOW
    top = LOW + PAIR * local
    tiles = final.shape[2] // LANES
    speeds_of(norms, speeds)
    theta_pass(phi, speeds, theta, LOW - 2, top + 1, first, count)
    update_pass(phi, speeds, theta, LOW - 1, top, first, count, store_final(final, rows))
    position = (
        lax.broadcasted_iota(jnp.int32, squares.shape, 0) * LANES
        + lax.broadcasted_iota(jnp.int32, squares.shape, 1)
    )

    def body(i, total):
        k = REACH + i
        acc = jnp.zeros((SUBLANES, LANES), F32)
        for t in range(tiles):
            diff = final[k, :, tile_of(t)] - final[k - 1, :, tile_of(t)]
            acc = acc + fold(diff * diff)
        amount = jnp.sum(jnp.sum(acc, axis=0, keepdims=True), axis=1, keepdims=True)
        return total + jnp.where(position == LOW + i + first, amount, 0.0)

    squares[...] = lax.fori_loop(0, PAIR * local, body, jnp.zeros(squares.shape, F32))


def store_final(final, rows):
    def store(k, t, value):
        if t < final.shape[2] // LANES:
            final[k - (LOW - REACH), :, tile_of(t)] = value[0:rows]

    return store


def rest_kernel(phi, norms, _, __, theta, final, speeds, *, count, local, rows, done):
    hi, _ = pair_position()
    first = hi * (PAIR * local) - LOW
    top = LOW + PAIR * local
    speeds_of(norms, speeds)
    for low, high in ((done + 1, LOW - 2), (top + 1, phi.shape[0] - done - 1)):
        theta_pass(phi, speeds, theta, low, high, first, count)
    for low, high in ((LOW - REACH, LOW - 1), (top, top + REACH + 1)):
        update_pass(phi, speeds, theta, low, high, first, count, store_final(final, rows))


def combine_kernel(bracket, window, squares, out, *scratch, count, own):
    hi, lo = pair_position()
    part = lo if own else 1 - lo
    whole, out = out, scratch[0] if own else out
    local, _, half = out.shape
    tiles = half // LANES
    begin = hi * (PAIR * local)
    position = (
        lax.broadcasted_iota(jnp.int32, squares.shape, 0) * LANES
        + lax.broadcasted_iota(jnp.int32, squares.shape, 1)
    )
    counted = (position >= 1) & (position < count)
    segments = jnp.where(counted, jnp.sqrt(squares[...] + EPSILON), 0.0)

    def total(value):
        return jnp.sum(jnp.sum(value, axis=0, keepdims=True), axis=1, keepdims=True)

    length = total(segments)
    weights = []
    for i in range(local):
        b = bracket[i]
        j = begin + part * local + i
        arc = total(jnp.where(position <= b, segments, 0.0))
        segment = total(jnp.where(position == b + 1, segments, 0.0))
        target = length * lax.convert_element_type(j, F32) / F32(count - 1)
        weights.append((target - arc) / segment)
    for i in range(local):
        at = bracket[i] - begin + REACH
        for t in range(tiles):
            base = window[at, :, tile_of(t)]
            out[i, :, tile_of(t)] = base + weights[i] * (window[at + 1, :, tile_of(t)] - base)
    if own:
        copy_half(out, whole, lo, scratch[1])


def copy_half(half_ref, whole, part, sem):
    half = half_ref.shape[2]
    copy = pltpu.make_async_copy(half_ref, whole.at[:, :, pl.ds(pl.multiple_of(part * half, LANES), half)], sem)
    copy.start()
    copy.wait()


def finish_kernel(whole_in, other, whole, sem):
    _, lo = pair_position()
    copy_half(other, whole, 1 - lo, sem)


def per_device(path, bracket):
    local, rows, columns = path.shape
    devices = lax.axis_size("img")
    count = local * devices
    half = columns // PAIR
    wide = half + LANES
    window = LOW + PAIR * local + HIGH
    if devices & (devices - 1) or ITERS != 2 or local != 2 * ITERS or count > SUBLANES * LANES or rows % SUBLANES:
        raise ValueError("unsupported sizes")
    shape = functools.partial(jax.ShapeDtypeStruct, dtype=F32)
    ahead = [(i, i + PAIR) for i in range(devices - PAIR)]
    back = [(target, source) for source, target in ahead]
    move = lambda value, up, down: lax.ppermute(
        value, "img",
        [p for p in ahead if p[0] % PAIR in up] + [p for p in back if p[0] % PAIR in down],
    )
    tiles = half // LANES
    message = lambda n: shape((n * tiles + 1, rows, LANES))
    first_chunk = CHUNKS[1]
    keep, send_first, send_second, shared, extra = call(
        pack_kernel,
        (message(local), message(first_chunk), message(local - first_chunk), message(SHARED), message(FAR - SHARED)),
        operands=1,
    )(path)
    recv = [swap_pairs(send_first), swap_pairs(send_second)]
    other_bracket = swap_pairs(bracket)
    near_early = move(keep, (1,), (0,))
    far_early = move(shared, (0,), (1,))
    near_late = [move(value, (0,), (1,)) for value in recv]
    far_late = move(call(far_kernel, message(FAR), operands=2)(*recv), (1,), (0,))
    far_extra = move(extra, (), (1,))
    rows_early = neighbour_rows(tiles, [keep] + recv + [near_early, near_late[0]])
    rows_late = neighbour_rows(tiles, [near_late[1], far_late, far_early, far_extra])
    held = shape((window, rows + 2 * EDGE, wide))
    lines = -(-window // SUBLANES) * SUBLANES
    norm_shape = shape((2, lines, LANES))
    operands = [keep] + recv + [near_early, near_late[0], rows_early]
    inside = PAIR * local + 2
    inside_lines = -(-inside // SUBLANES) * SUBLANES
    phi, drift, norms = call(
        functools.partial(inner_kernel, count=count, local=local), (held, held, shape((2, inside_lines, LANES))),
        operands=len(operands),
    )(*operands)
    norms = small_sum(norms, (1,))
    own_norms = norms[:, 1 : inside - 1]
    low_norms = lax.ppermute(own_norms, "img", ahead)
    high_norms = lax.ppermute(own_norms, "img", back)
    state = call(
        functools.partial(middle_inner_kernel, count=count, local=local, rows=rows),
        (held, held, held, held, norm_shape), scratch=[pltpu.VMEM((inside_lines, LANES), F32)],
        operands=3, aliases={0: 0, 1: 1},
    )(phi, drift, norms)
    pad = jnp.zeros((2, lines - window, LANES), F32)
    norms = jnp.concatenate([low_norms[:, PAIR * local - LOW :], own_norms, high_norms[:, :HIGH], pad], axis=1)
    operands = [norms, near_late[1], far_early, far_extra, far_late, rows_late]
    _, _, phi, drift, norms = call(
        functools.partial(middle_outer_kernel, count=count, local=local),
        (held, held, held, held, norm_shape), scratch=[pltpu.VMEM((lines, LANES), F32)],
        operands=len(operands) + len(state), aliases={len(operands) + i: i for i in range(len(state))},
    )(*operands, *state)
    scratch = [pltpu.VMEM((lines, LANES), F32)]
    norms = small_sum(norms, (1,))
    final_shape = shape((PAIR * local + 2 * REACH + 1, rows, half))
    final, squares, theta = call(
        functools.partial(last_kernel, count=count, local=local, rows=rows),
        (final_shape, shape((SUBLANES, LANES)), held),
        scratch=scratch, operands=3, aliases={1: 2},
    )(phi, drift, norms)
    _, final = call(
        functools.partial(rest_kernel, count=count, local=local, rows=rows, done=2 * (ITERS - 1)),
        (held, final_shape), scratch=scratch, operands=4, aliases={2: 0, 3: 1},
    )(phi, norms, theta, final)
    steps = []
    step = 1
    while step < devices:
        steps.append(step)
        step *= 2
    squares = small_sum(squares, steps)
    half_block = (local, rows, half)
    whole = shape((local, rows, columns))
    in_smem, in_vmem, in_hbm = (pl.BlockSpec(memory_space=m) for m in (pltpu.SMEM, pltpu.VMEM, pl.ANY))
    other = swap_pairs(
        call(functools.partial(combine_kernel, count=count, own=False), shape(half_block), smem=1, operands=2)(
            other_bracket, final, squares
        )
    )
    mine = pl.pallas_call(
        functools.partial(combine_kernel, count=count, own=True),
        out_shape=whole,
        in_specs=[in_smem, in_vmem, in_vmem],
        out_specs=in_hbm,
        scratch_shapes=[pltpu.VMEM(half_block, F32), pltpu.SemaphoreType.DMA],
        compiler_params=pltpu.CompilerParams(vmem_limit_bytes=VMEM_LIMIT),
    )(bracket, final, squares)
    return pl.pallas_call(
        finish_kernel,
        out_shape=whole,
        in_specs=[in_hbm, in_vmem],
        out_specs=in_hbm,
        scratch_shapes=[pltpu.SemaphoreType.DMA],
        input_output_aliases={0: 0},
        compiler_params=pltpu.CompilerParams(vmem_limit_bytes=VMEM_LIMIT),
    )(mine, other)


def solution(mesh):
    return jax.shard_map(
        per_device,
        mesh=mesh,
        in_specs=(P(("groups", "img"), "space", None), P(("groups", "img"))),
        out_specs=P(("groups", "img"), "space", None),
        check_vma=False,
    )
```

```python
import functools

import jax
import jax.numpy as jnp
from jax import lax
from jax.experimental import pallas as pl
from jax.experimental.pallas import tpu as pltpu
from jax.sharding import PartitionSpec as P


REACH = 2
ITERS = 2
TIME_STEP = 0.002
EPSILON = 1e-06

LANES = 128
SUBLANES = 8
PAIR = 2
LOW = 2 * ITERS + REACH
HIGH = 2 * ITERS + REACH + 1
FAR = 3
SHARED = 2
EDGE = 2 * ITERS
CHUNKS = (0, 2)
VMEM_LIMIT = 4 * 1024 * 1024

F32 = jnp.float32


def call(kernel, out_shapes, scratch=(), smem=0, operands=0, aliases=None):
    specs = [pl.BlockSpec(memory_space=pltpu.SMEM)] * smem
    specs += [pl.BlockSpec(memory_space=pltpu.VMEM)] * operands
    return pl.pallas_call(
        kernel,
        out_shape=out_shapes,
        in_specs=specs,
        out_specs=jax.tree.map(lambda _: pl.BlockSpec(memory_space=pltpu.VMEM), out_shapes),
        scratch_shapes=list(scratch),
        input_output_aliases=aliases or {},
        compiler_params=pltpu.CompilerParams(vmem_limit_bytes=VMEM_LIMIT),
    )


def pair_position():
    index = lax.axis_index("img")
    return lax.div(index, PAIR), lax.rem(index, PAIR)


def swap_pairs(value):
    count = lax.axis_size("img")
    return lax.ppermute(value, "img", [(i, i ^ 1) for i in range(count)])


def small_sum(value, steps):
    size = lax.axis_size("space")
    if size & (size - 1) == 0:
        step = 1
        while step < size:
            value = value + lax.ppermute(value, "space", [(i, i ^ step) for i in range(size)])
            step *= 2
    else:
        value = lax.psum(value, "space")
    count = lax.axis_size("img")
    for step in steps:
        other = lax.ppermute(value, "img", [(i, i ^ step) for i in range(count)])
        value = value + other
    return value


def tile_of(t):
    return slice(t * LANES, (t + 1) * LANES)


def images_of(message, tiles):
    return (message.shape[0] - 1) // tiles


def edge_tile(message, i):
    return pltpu.roll(message[message.shape[0] - 1], LANES - EDGE - 2 * EDGE * i, 1)


def pack_edges(tiles):
    lane = lax.broadcasted_iota(jnp.int32, tiles[0].shape, 1)
    packed = jnp.zeros(tiles[0].shape, F32)
    for i, tile in enumerate(tiles):
        mine = (lane >= 2 * EDGE * i) & (lane < 2 * EDGE * (i + 1))
        packed = jnp.where(mine, pltpu.roll(tile, EDGE + 2 * EDGE * i, 1), packed)
    return packed


def pick_kernel(*refs):
    *messages, picked = refs
    tiles = picked.shape[2] // LANES - 1
    at = 0
    for message in messages:
        for i in range(images_of(message, tiles)):
            for t in range(tiles + 1):
                tile = message[i * tiles + t] if t < tiles else edge_tile(message, i)
                picked[at, 0:EDGE, tile_of(t)] = tile[0:EDGE]
                picked[at, EDGE:, tile_of(t)] = tile[tile.shape[0] - EDGE :]
            at += 1


def neighbour_rows(tiles, blocks):
    size = lax.axis_size("space")
    count = sum(images_of(block, tiles) for block in blocks)
    picked = call(
        pick_kernel, jax.ShapeDtypeStruct((count, 2 * EDGE, (tiles + 1) * LANES), F32), operands=len(blocks)
    )(*blocks)
    if size == 1:
        return picked
    if size == 2:
        return lax.ppermute(picked, "space", [(0, 1), (1, 0)])
    after = lax.ppermute(picked[:, :EDGE], "space", [(i, (i - 1) % size) for i in range(size)])
    before = lax.ppermute(picked[:, EDGE:], "space", [(i, (i + 1) % size) for i in range(size)])
    return jnp.concatenate([after, before], axis=1)


def pack_kernel(x_ref, *refs, sent):
    _, lo = pair_position()
    local, rows, columns = x_ref.shape
    half = columns // PAIR
    tiles = half // LANES
    lane = lax.broadcasted_iota(jnp.int32, (rows, LANES), 1)

    def fill(ref, part, chosen):
        begin = part * half
        right = pl.multiple_of((1 - part) * half, LANES)
        left = pl.multiple_of((1 - part) * half + half - LANES, LANES)
        edges = []
        for i, q in enumerate(chosen):
            k = jnp.where(lo == 0, q, local - 1 - q)
            for t in range(tiles):
                ref[i * tiles + t] = x_ref[k, :, pl.ds(pl.multiple_of(begin + t * LANES, LANES), LANES)]
            edges.append(
                jnp.where(lane < LANES // 2, x_ref[k, :, pl.ds(right, LANES)], x_ref[k, :, pl.ds(left, LANES)])
            )
        ref[len(chosen) * tiles] = pack_edges(edges)

    if sent:
        chosen = (range(CHUNKS[1]), range(CHUNKS[1], local))
    else:
        chosen = (range(local), range(local - SHARED, local), range(local - FAR, local - SHARED))
    for ref, images in zip(refs, chosen):
        fill(ref, 1 - lo if sent else lo, images)


def far_kernel(first, second, out):
    tiles = (first.shape[0] - 1) // CHUNKS[1]
    local = CHUNKS[1] + images_of(second, tiles)
    edges = []
    for i, q in enumerate(range(local - FAR, local)):
        source, at = (first, q) if q < CHUNKS[1] else (second, q - CHUNKS[1])
        for t in range(tiles):
            out[i * tiles + t] = source[at * tiles + t]
        edges.append(edge_tile(source, at))
    out[FAR * tiles] = pack_edges(edges)


def sum_of_neighbours(load, tiles, rows, use):
    lane = lax.broadcasted_iota(jnp.int32, (rows, LANES), 1)
    is_first, is_last = lane == 0, lane == LANES - 1
    center = load(0)
    from_left = pltpu.roll(load(tiles - 1), 1, 1)
    to_left = pltpu.roll(center, LANES - 1, 1)
    for t in range(tiles):
        following = load((t + 1) % tiles)
        shifted = pltpu.roll(center, 1, 1)
        next_to_left = pltpu.roll(following, LANES - 1, 1)
        west = jnp.where(is_first, from_left, shifted)
        east = jnp.where(is_last, next_to_left, to_left)
        north = pltpu.roll(center, 1, 0)
        south = pltpu.roll(center, rows - 1, 0)
        use(t, center, (north + south) + (west + east))
        center, from_left, to_left = following, shifted, next_to_left


def neighbours_of(k, first, count):
    gid = k + first
    is_first, is_last = gid == 0, gid == count - 1
    before = jnp.where(is_first, k, k - 1)
    after = jnp.where(is_last, k, k + 1)
    stretch = jnp.where(is_first | is_last, F32(count - 1), F32((count - 1) / 2.0))
    return before, after, stretch


def fold(value):
    return jnp.sum(value.reshape(-1, SUBLANES, LANES), axis=0)


def drift_pass(phi, drift, norms, low, high, first, count, own_rows, shift=0):
    rows = phi.shape[1]
    tiles = phi.shape[2] // LANES

    def body(k, carry):
        before, after, stretch = neighbours_of(k, first, count)
        sums = [jnp.zeros((SUBLANES, LANES), F32), jnp.zeros((SUBLANES, LANES), F32)]

        def use(t, center, total):
            force = total - center * (3.0 + center * center)
            drift[k, :, tile_of(t)] = force
            if t < tiles - 1 and norms is not None:
                step = phi[after, 0:own_rows, tile_of(t)] - phi[before, 0:own_rows, tile_of(t)]
                own = force[0:own_rows]
                sums[0] = sums[0] + fold(own * own)
                sums[1] = sums[1] + fold(step * step)

        sum_of_neighbours(lambda t: phi[k, :, tile_of(t)], tiles, rows, use)
        if norms is not None:
            norms[0, pl.ds(k - shift, 1), :] = jnp.sum(sums[0], axis=0, keepdims=True)
            norms[1, pl.ds(k - shift, 1), :] = jnp.sum(sums[1], axis=0, keepdims=True) * (stretch * stretch)
        return carry

    lax.fori_loop(low, high, body, 0)


def speeds_of(norms, speeds):
    force = jnp.sum(norms[0], axis=1, keepdims=True)
    path = jnp.sum(norms[1], axis=1, keepdims=True)
    value = jnp.sqrt(force + EPSILON) / jnp.sqrt(path + EPSILON)
    speeds[...] = jnp.broadcast_to(value, speeds.shape)


def theta_pass(phi, speeds, theta, low, high, first, count, shift=0):
    tiles = phi.shape[2] // LANES

    def body(k, carry):
        before, after, stretch = neighbours_of(k, first, count)
        scale = speeds[pl.ds(k - shift, 1), :] * stretch
        for t in range(tiles):
            cols = tile_of(t)
            theta[k, :, cols] = scale * (phi[after, :, cols] - phi[before, :, cols]) - theta[k, :, cols]
        return carry

    lax.fori_loop(low, high, body, 0)


def update_pass(phi, speeds, theta, low, high, first, count, store, shift=0):
    rows = phi.shape[1]
    tiles = phi.shape[2] // LANES

    def body(k, carry):
        before, after, stretch = neighbours_of(k, first, count)
        scale = speeds[pl.ds(k - shift, 1), :] * stretch
        gid = k + first
        inside = (gid > 0) & (gid < count - 1)

        def use(t, center, total):
            cols = tile_of(t)
            value = phi[k, :, cols]
            descent = (
                scale * (theta[after, :, cols] - theta[before, :, cols])
                + total
                - (3.0 * center) * (1.0 + value * value)
            )
            store(k, t, jnp.where(inside, value + TIME_STEP * descent, value))

        sum_of_neighbours(lambda t: theta[k, :, tile_of(t)], tiles, rows, use)
        return carry

    lax.fori_loop(low, high, body, 0)


def place(phi, at, message, i, edge_rows):
    rows = message.shape[1]
    tiles = phi.shape[2] // LANES - 1
    for t in range(tiles):
        phi[at, 0:rows, tile_of(t)] = message[i * tiles + t]
    phi[at, 0:rows, tile_of(tiles)] = edge_tile(message, i)
    phi[at, rows:, :] = edge_rows


def inner_kernel(*refs, count, local):
    keep, first_recv, second_recv, near_early, near_late, edge_rows, phi, drift, norms = refs
    rows = keep.shape[1]
    hi, lo = pair_position()
    first = hi * (PAIR * local) - LOW
    top = LOW + PAIR * local
    half = CHUNKS[1]

    def own_at(part, q):
        return LOW + part * local + jnp.where(part == 0, q, local - 1 - q)

    for q in range(local):
        place(phi, own_at(lo, q), keep, q, edge_rows[q])
        source, at = (first_recv, q) if q < half else (second_recv, q - half)
        place(phi, own_at(1 - lo, q), source, at, edge_rows[local + q])
        low_at, high_at = LOW - 1 - q, top + q
        place(phi, jnp.where(lo == 1, low_at, high_at), near_early, q, edge_rows[2 * local + q])
        if q < half:
            place(phi, jnp.where(lo == 1, high_at, low_at), near_late, q, edge_rows[3 * local + q])
    drift_pass(phi, drift, norms, LOW - 1, top + 1, first, count, rows, LOW - 1)


def middle_inner_kernel(_, __, norms, phi, theta, new_phi, new_drift, new_norms, speeds, *, count, local, rows):
    hi, _ = pair_position()
    first = hi * (PAIR * local) - LOW
    top = LOW + PAIR * local
    speeds_of(norms, speeds)
    theta_pass(phi, speeds, theta, LOW - 1, top + 1, first, count, LOW - 1)

    def store(k, t, value):
        new_phi[k, :, tile_of(t)] = value

    update_pass(phi, speeds, theta, LOW, top, first, count, store, LOW - 1)
    new_norms[...] = jnp.zeros(new_norms.shape, F32)
    drift_pass(new_phi, new_drift, new_norms, LOW + 1, top - 1, first, count, rows)


def middle_outer_kernel(norms, near_late, far_early, far_extra, far_late, rows_late, *refs, count, local):
    phi, theta, new_phi, new_drift, new_norms, speeds = refs[5:]
    rows = near_late.shape[1]
    hi, lo = pair_position()
    first = hi * (PAIR * local) - LOW
    top = LOW + PAIR * local
    window = phi.shape[0]
    done = CHUNKS[-1]
    for q in range(done, local):
        place(phi, jnp.where(lo == 1, top + q, LOW - 1 - q), near_late, q - done, rows_late[q - done])
    for i in range(FAR):
        low_at, high_at = LOW - 1 - local - i, top + local + i
        at = FAR - 1 - i
        late = (far_late, at, rows_late.at[local - done + at])
        if i < SHARED:
            early = (far_early, SHARED - 1 - i, rows_late.at[local - done + FAR + SHARED - 1 - i])
        else:
            early = (far_extra, FAR - 1 - i, rows_late.at[local - done + FAR + FAR - 1 - i + SHARED])

        @pl.when(lo == 1)
        def _():
            for position, (message, index, edge) in ((high_at, early), (low_at, late)):
                if 0 <= position < window:
                    place(phi, position, message, index, edge[...])

        @pl.when(lo == 0)
        def _():
            for position, (message, index, edge) in ((high_at, late), (low_at, early)):
                if 0 <= position < window:
                    place(phi, position, message, index, edge[...])

    def store(k, t, value):
        new_phi[k, :, tile_of(t)] = value

    speeds_of(norms, speeds)
    for low, high in ((1, LOW - 1), (top + 1, window - 1)):
        drift_pass(phi, theta, None, low, high, first, count, rows)
        theta_pass(phi, speeds, theta, low, high, first, count)
    for low, high in ((2, LOW), (top, window - 2)):
        update_pass(phi, speeds, theta, low, high, first, count, store)
    for low, high in ((3, LOW + 1), (top - 1, window - 3)):
        drift_pass(new_phi, new_drift, new_norms, low, high, first, count, rows)


def last_kernel(phi, _, norms, final, squares, theta, speeds, *, count, local, rows):
    hi, _ = pair_position()
    first = hi * (PAIR * local) - LOW
    top = LOW + PAIR * local
    tiles = final.shape[2] // LANES
    speeds_of(norms, speeds)
    theta_pass(phi, speeds, theta, LOW - 2, top + 1, first, count)
    update_pass(phi, speeds, theta, LOW - 1, top, first, count, store_final(final, rows))
    position = (
        lax.broadcasted_iota(jnp.int32, squares.shape, 0) * LANES
        + lax.broadcasted_iota(jnp.int32, squares.shape, 1)
    )

    def body(i, total):
        k = REACH + i
        acc = jnp.zeros((SUBLANES, LANES), F32)
        for t in range(tiles):
            diff = final[k, :, tile_of(t)] - final[k - 1, :, tile_of(t)]
            acc = acc + fold(diff * diff)
        amount = jnp.sum(jnp.sum(acc, axis=0, keepdims=True), axis=1, keepdims=True)
        return total + jnp.where(position == LOW + i + first, amount, 0.0)

    squares[...] = lax.fori_loop(0, PAIR * local, body, jnp.zeros(squares.shape, F32))


def store_final(final, rows):
    def store(k, t, value):
        if t < final.shape[2] // LANES:
            final[k - (LOW - REACH), :, tile_of(t)] = value[0:rows]

    return store


def rest_kernel(phi, norms, _, __, theta, final, speeds, *, count, local, rows, done):
    hi, _ = pair_position()
    first = hi * (PAIR * local) - LOW
    top = LOW + PAIR * local
    speeds_of(norms, speeds)
    for low, high in ((done + 1, LOW - 2), (top + 1, phi.shape[0] - done - 1)):
        theta_pass(phi, speeds, theta, low, high, first, count)
    for low, high in ((LOW - REACH, LOW - 1), (top, top + REACH + 1)):
        update_pass(phi, speeds, theta, low, high, first, count, store_final(final, rows))


def combine_kernel(bracket, window, squares, out, *scratch, count, own):
    hi, lo = pair_position()
    part = lo if own else 1 - lo
    whole, out = out, scratch[0] if own else out
    local, _, half = out.shape
    tiles = half // LANES
    begin = hi * (PAIR * local)
    position = (
        lax.broadcasted_iota(jnp.int32, squares.shape, 0) * LANES
        + lax.broadcasted_iota(jnp.int32, squares.shape, 1)
    )
    counted = (position >= 1) & (position < count)
    segments = jnp.where(counted, jnp.sqrt(squares[...] + EPSILON), 0.0)

    def total(value):
        return jnp.sum(jnp.sum(value, axis=0, keepdims=True), axis=1, keepdims=True)

    length = total(segments)
    weights = []
    for i in range(local):
        b = bracket[i]
        j = begin + part * local + i
        arc = total(jnp.where(position <= b, segments, 0.0))
        segment = total(jnp.where(position == b + 1, segments, 0.0))
        target = length * lax.convert_element_type(j, F32) / F32(count - 1)
        weights.append((target - arc) / segment)
    for i in range(local):
        at = bracket[i] - begin + REACH
        for t in range(tiles):
            base = window[at, :, tile_of(t)]
            out[i, :, tile_of(t)] = base + weights[i] * (window[at + 1, :, tile_of(t)] - base)
    if own:
        copy_half(out, whole, lo, scratch[1])


def copy_half(half_ref, whole, part, sem):
    half = half_ref.shape[2]
    copy = pltpu.make_async_copy(half_ref, whole.at[:, :, pl.ds(pl.multiple_of(part * half, LANES), half)], sem)
    copy.start()
    copy.wait()


def finish_kernel(whole_in, other, whole, sem):
    _, lo = pair_position()
    copy_half(other, whole, 1 - lo, sem)


def per_device(path, bracket):
    local, rows, columns = path.shape
    devices = lax.axis_size("img")
    count = local * devices
    half = columns // PAIR
    wide = half + LANES
    window = LOW + PAIR * local + HIGH
    if devices & (devices - 1) or ITERS != 2 or local != 2 * ITERS or count > SUBLANES * LANES or rows % SUBLANES:
        raise ValueError("unsupported sizes")
    shape = functools.partial(jax.ShapeDtypeStruct, dtype=F32)
    ahead = [(i, i + PAIR) for i in range(devices - PAIR)]
    back = [(target, source) for source, target in ahead]
    move = lambda value, up, down: lax.ppermute(
        value, "img",
        [p for p in ahead if p[0] % PAIR in up] + [p for p in back if p[0] % PAIR in down],
    )
    tiles = half // LANES
    message = lambda n: shape((n * tiles + 1, rows, LANES))
    first_chunk = CHUNKS[1]
    send_first, send_second = call(
        functools.partial(pack_kernel, sent=True), (message(first_chunk), message(local - first_chunk)), operands=1
    )(path)
    keep, shared, extra = call(
        functools.partial(pack_kernel, sent=False),
        (message(local), message(SHARED), message(FAR - SHARED)), operands=1,
    )(path)
    recv = [swap_pairs(send_first), swap_pairs(send_second)]
    other_bracket = swap_pairs(bracket)
    near_early = move(keep, (1,), (0,))
    far_early = move(shared, (0,), (1,))
    near_late = [move(value, (0,), (1,)) for value in recv]
    far_late = move(call(far_kernel, message(FAR), operands=2)(*recv), (1,), (0,))
    far_extra = move(extra, (), (1,))
    rows_early = neighbour_rows(tiles, [keep] + recv + [near_early, near_late[0]])
    rows_late = neighbour_rows(tiles, [near_late[1], far_late, far_early, far_extra])
    held = shape((window, rows + 2 * EDGE, wide))
    lines = -(-window // SUBLANES) * SUBLANES
    norm_shape = shape((2, lines, LANES))
    operands = [keep] + recv + [near_early, near_late[0], rows_early]
    inside = PAIR * local + 2
    inside_lines = -(-inside // SUBLANES) * SUBLANES
    phi, drift, norms = call(
        functools.partial(inner_kernel, count=count, local=local), (held, held, shape((2, inside_lines, LANES))),
        operands=len(operands),
    )(*operands)
    norms = small_sum(norms, (1,))
    own_norms = norms[:, 1 : inside - 1]
    low_norms = lax.ppermute(own_norms, "img", ahead)
    high_norms = lax.ppermute(own_norms, "img", back)
    state = call(
        functools.partial(middle_inner_kernel, count=count, local=local, rows=rows),
        (held, held, held, held, norm_shape), scratch=[pltpu.VMEM((inside_lines, LANES), F32)],
        operands=3, aliases={0: 0, 1: 1},
    )(phi, drift, norms)
    pad = jnp.zeros((2, lines - window, LANES), F32)
    norms = jnp.concatenate([low_norms[:, PAIR * local - LOW :], own_norms, high_norms[:, :HIGH], pad], axis=1)
    operands = [norms, near_late[1], far_early, far_extra, far_late, rows_late]
    _, _, phi, drift, norms = call(
        functools.partial(middle_outer_kernel, count=count, local=local),
        (held, held, held, held, norm_shape), scratch=[pltpu.VMEM((lines, LANES), F32)],
        operands=len(operands) + len(state), aliases={len(operands) + i: i for i in range(len(state))},
    )(*operands, *state)
    scratch = [pltpu.VMEM((lines, LANES), F32)]
    norms = small_sum(norms, (1,))
    final_shape = shape((PAIR * local + 2 * REACH + 1, rows, half))
    final, squares, theta = call(
        functools.partial(last_kernel, count=count, local=local, rows=rows),
        (final_shape, shape((SUBLANES, LANES)), held),
        scratch=scratch, operands=3, aliases={1: 2},
    )(phi, drift, norms)
    _, final = call(
        functools.partial(rest_kernel, count=count, local=local, rows=rows, done=2 * (ITERS - 1)),
        (held, final_shape), scratch=scratch, operands=4, aliases={2: 0, 3: 1},
    )(phi, norms, theta, final)
    steps = []
    step = 1
    while step < devices:
        steps.append(step)
        step *= 2
    squares = small_sum(squares, steps)
    half_block = (local, rows, half)
    whole = shape((local, rows, columns))
    in_smem, in_vmem, in_hbm = (pl.BlockSpec(memory_space=m) for m in (pltpu.SMEM, pltpu.VMEM, pl.ANY))
    other = swap_pairs(
        call(functools.partial(combine_kernel, count=count, own=False), shape(half_block), smem=1, operands=2)(
            other_bracket, final, squares
        )
    )
    mine = pl.pallas_call(
        functools.partial(combine_kernel, count=count, own=True),
        out_shape=whole,
        in_specs=[in_smem, in_vmem, in_vmem],
        out_specs=in_hbm,
        scratch_shapes=[pltpu.VMEM(half_block, F32), pltpu.SemaphoreType.DMA],
        compiler_params=pltpu.CompilerParams(vmem_limit_bytes=VMEM_LIMIT),
    )(bracket, final, squares)
    return pl.pallas_call(
        finish_kernel,
        out_shape=whole,
        in_specs=[in_hbm, in_vmem],
        out_specs=in_hbm,
        scratch_shapes=[pltpu.SemaphoreType.DMA],
        input_output_aliases={0: 0},
        compiler_params=pltpu.CompilerParams(vmem_limit_bytes=VMEM_LIMIT),
    )(mine, other)


def solution(mesh):
    return jax.shard_map(
        per_device,
        mesh=mesh,
        in_specs=(P(("groups", "img"), "space", None), P(("groups", "img"))),
        out_specs=P(("groups", "img"), "space", None),
        check_vma=False,
    )
```
